32 devices in a mesh: groups: 2 (over y), az: 4 (over z), rg: 2 (over x), acq: 2 (over core).
Axes of the slice: x: 2, y: 2, z: 4, core: 2. Of those that a mesh axis runs over, the one named last changes fastest.
Arguments:
- image_stack: bfloat16 [2, 64, 32, 4, 256], P(None, ('az', 'acq'), 'groups', 'rg'), parts along dimension 2, may hold values from -12 to 12
- steering: bfloat16 [4, 2, 64, 512], P('rg'), as said below
- wiener_filter: bfloat16 [4, 2, 64, 64], P('rg'), may hold values from -0.5 to 0.5
- range_group: int32 [4], P('rg'), may hold values from 0 to 3, as said below
- lay_list: int32 [32, 4, 32], P(('groups', 'az', 'acq'), 'rg'), parts along dimension 0, may hold values from 0 to 255, as said below
- lay_count: int32 [32, 4], P(('groups', 'az', 'acq'), 'rg'), parts along dimension 0, may hold values from 0 to 32, as said below
Outputs:
- power: bfloat16 [32, 4, 512, 256], P(('groups', 'az', 'acq'), 'rg'), parts along dimension 0
The draws below stay inside these ranges and needn't reach their ends.
There are 2 independent parts, one for each index of `groups`. The reference program is written for one: setup_inputs(seed, part) draws one part's arguments, and reference() takes and returns one part's arrays. A program takes and returns all parts, laid end to end along the dimension named above; an argument that names none is the same for every part. Nothing has to cross between parts.
Inputs may be any that keep to these rules, and one draw needn't show every extreme that they name: `lay_list`: within one block the 32 entries are distinct pixels. The first lay_count entries of a block's list are its layover pixels; some block has 32. `range_group`: range block r belongs to a group from (r // 2) * 2 to (r // 2) * 2 + 1. `steering`: every complex entry has modulus 1 / sqrt(512) up to rounding.
All inputs are finite; a program needn't handle non-finite values.
Results may differ from the reference program's by a relative error of at most 0.0075.
Values may be sent and summed in bfloat16 or wider, within the bound.
No kernel may reach another device: no remote copies, remote signals or barrier semaphores. Data moves between devices by JAX's collectives and lax.ppermute only.
A program may use at most 64 MiB of HBM per device.

```python
import math
import jax
import jax.numpy as jnp
from jax import lax

K = 64
E = 512
BLK = 256
LMAX = 32
GRP_DEV = 2
ITERS = 8
AZB_DEV = 2
RGB_DEV = 2
AZB = 16
RGB = 4
NGRP = 4


def draw_steering(key, part):
    phases = jax.random.uniform(key, (NGRP, K, E), jnp.float32, -math.pi, math.pi)
    scale = 1.0 / math.sqrt(E)
    return (jnp.stack([jnp.cos(phases), jnp.sin(phases)], axis=1) * scale).astype(jnp.bfloat16)


def draw_range_group(key, part):
    wide_values = jax.random.randint(key, (RGB,), 0, 1048576, dtype=jnp.int32)
    offset = wide_values % GRP_DEV
    return jnp.arange(RGB, dtype=jnp.int32) // RGB_DEV * GRP_DEV + offset


def draw_lay_list(key, part):
    scores = jax.random.randint(jax.random.fold_in(key, 21), (AZB, RGB, BLK), 0, 1048576, dtype=jnp.int32)
    scores = scores * BLK + jnp.arange(BLK, dtype=jnp.int32)
    ordering = jnp.argsort(scores, axis=-1)
    return ordering[:, :, :LMAX].astype(jnp.int32)


def draw_lay_count(key, part):
    urban_flag = jax.random.randint(jax.random.fold_in(key, 31), (AZB // AZB_DEV, RGB // RGB_DEV), 0, 4, dtype=jnp.int32) == 0
    urban_flag = jnp.repeat(jnp.repeat(urban_flag, AZB_DEV, axis=0), RGB_DEV, axis=1)
    heavy_count = jax.random.randint(jax.random.fold_in(key, 32), (AZB, RGB), LMAX // 2, LMAX + 1, dtype=jnp.int32)
    light_count = jax.random.randint(jax.random.fold_in(key, 33), (AZB, RGB), 0, LMAX // 8 + 1, dtype=jnp.int32)
    counts = jnp.where(urban_flag, heavy_count, light_count)
    return counts.at[0, 0].set(LMAX)


def block_levels(key, extent, shards, smallest, high):
    level, own = 1.0, jax.random.fold_in(key, 6)
    for axis_at, shards_of in shards:
        heights = jnp.exp(jax.random.uniform(jax.random.fold_in(own, axis_at), (shards_of,), jnp.float32, smallest / len(shards), high / len(shards)))
        level = level * jnp.repeat(heights, extent[axis_at] // shards_of).reshape([-1 if axis == axis_at else 1 for axis in range(len(extent))])
    return level


def gaussian(rng, extent, spread, reach, shards=(), kind=jnp.bfloat16):
    entries = spread * jax.random.normal(rng, extent, jnp.float32)
    if shards:
        entries = entries * block_levels(rng, extent, shards, -0.22, 0.18)
    return jnp.clip(entries, -reach, reach).astype(kind)


def setup_inputs(seed: int = 0, part: int = 0) -> dict:
    splits = jax.random.split(jax.random.key(seed), 7)
    part_keys = jax.random.split(jax.random.fold_in(splits[6], part), 7)
    return {
        "image_stack": gaussian(part_keys[0], (2, K, AZB, RGB, BLK), 2.0, 12.0, ((1, 8), (3, 2))),
        "steering": draw_steering(jax.random.fold_in(splits[6], 71), part),
        "wiener_filter": gaussian(splits[2], (NGRP, 2, K, K), (2 * K) ** -0.5, 0.5, ((0, 2),)),
        "range_group": draw_range_group(jax.random.fold_in(splits[6], 71), part),
        "lay_list": draw_lay_list(jax.random.fold_in(jax.random.fold_in(splits[6], part), 71), part),
        "lay_count": draw_lay_count(jax.random.fold_in(jax.random.fold_in(splits[6], part), 71), part),
    }


STEP_SIZE = 0.5
SHRINK = 0.25

def complex_block(complex_parts):
    real_part = complex_parts[0]
    imag_part = complex_parts[1]
    upper = jnp.concatenate([real_part, -imag_part], axis=1)
    lower = jnp.concatenate([imag_part, real_part], axis=1)
    return jnp.concatenate([upper, lower], axis=0)

def ista_power(lane_data, operator):
    target = lane_data.astype(jnp.float32)
    elevation = operator.shape[1] // 2

    def sweep(sweep_index, estimate):
        rounded = estimate.astype(jnp.bfloat16)
        predicted = jnp.dot(rounded, operator.T, preferred_element_type=jnp.float32)
        misfit = (target - predicted).astype(jnp.bfloat16)
        update = estimate + STEP_SIZE * jnp.dot(misfit, operator, preferred_element_type=jnp.float32)
        magnitude = update[:, :elevation] ** 2 + update[:, elevation:] ** 2
        factor = jnp.maximum(1.0 - SHRINK * lax.rsqrt(jnp.maximum(magnitude, SHRINK * SHRINK)), 0.0)
        return update * jnp.concatenate([factor, factor], axis=1)
    start = jnp.zeros((lane_data.shape[0], 2 * elevation), jnp.float32)
    estimate = lax.fori_loop(0, ITERS, sweep, start)
    return (estimate[:, :elevation] ** 2 + estimate[:, elevation:] ** 2).astype(jnp.bfloat16)

def reference(image_stack, steering, wiener_filter, range_group, lay_list, lay_count):

    def column_power(column):
        group_id = range_group[column]
        operator = complex_block(lax.dynamic_index_in_dim(steering, group_id, 0, keepdims=False))
        filter_matrix = complex_block(lax.dynamic_index_in_dim(wiener_filter, group_id, 0, keepdims=False))
        block_data = lax.dynamic_index_in_dim(image_stack, column, 3, keepdims=False).reshape(2 * K, AZB, BLK)
        filtered = jnp.einsum('ij,jap->iap', filter_matrix.astype(jnp.float32), block_data.astype(jnp.float32)).astype(jnp.bfloat16)
        beamed = jnp.einsum('ie,iap->aep', operator.astype(jnp.float32), filtered.astype(jnp.float32))
        wiener_power = beamed[:, :E] ** 2 + beamed[:, E:] ** 2
        listed = lax.dynamic_index_in_dim(lay_list, column, 1, keepdims=False)
        live_count = lax.dynamic_index_in_dim(lay_count, column, 1, keepdims=False)
        usable = jnp.arange(LMAX, dtype=jnp.int32)[None, :] < live_count[:, None]
        chosen = ((listed[:, :, None] == jnp.arange(BLK, dtype=jnp.int32)[None, None, :]) & usable[:, :, None]).astype(jnp.float32)
        lane_data = jnp.einsum('alp,iap->ali', chosen, block_data.astype(jnp.float32)).astype(jnp.bfloat16).reshape(AZB * LMAX, 2 * K)
        lay_power = ista_power(lane_data, operator).reshape(AZB, LMAX, E)
        placed = jnp.einsum('alp,ale->aep', chosen, lay_power.astype(jnp.float32))
        covered = lax.optimization_barrier(jnp.sum(chosen, axis=1))
        return jnp.where(covered[:, None, :] > 0.5, placed, wiener_power).astype(jnp.bfloat16)
    columns = lax.map(column_power, jnp.arange(RGB, dtype=jnp.int32))
    return jnp.transpose(columns, (1, 0, 2, 3))
```

```python
import jax
import jax.numpy as jnp
from jax import lax
from jax.experimental import pallas as pl
from jax.experimental.pallas import tpu as pltpu
from jax.sharding import PartitionSpec as P

ITERS = 8
STEP_SIZE = 0.5
SHRINK = 0.25
LANES = 128
F32 = jnp.float32
BF16 = jnp.bfloat16

VMEM = pl.BlockSpec(memory_space=pltpu.VMEM)
SMEM = pl.BlockSpec(memory_space=pltpu.SMEM)
ANY = pl.BlockSpec(memory_space=pl.ANY)


def dot(a, b, contract=(1, 0)):
    return lax.dot_general(
        a, b, (((contract[0],), (contract[1],)), ((), ())), preferred_element_type=F32
    )


def relay_kernel(coords, x_ref, *refs):
    chunks, sem = refs[:-1], refs[-1]
    halves, acq_share = x_ref.shape[:2]
    per_chip = chunks[0].shape[0]
    copies = []
    for d, chunk in enumerate(chunks):
        first = coords[d] * per_chip
        for half in range(halves):
            for acq in range(acq_share):
                copies.append(
                    pltpu.make_async_copy(
                        x_ref.at[half, acq, pl.ds(first, per_chip)],
                        chunk.at[:, half, :, acq],
                        sem,
                    )
                )
    for copy in copies:
        copy.start()
    for copy in copies:
        copy.wait()


def prepare_kernel(
    acq_share, groups, counts, list_ref, steer_ref, filter_ref,
    half_op_ref, op_t_ref, wiener_ref, select_ref, chosen_ref, clear_ref, fmat_ref,
):
    acquisitions, elevation = steer_ref.shape[2:]
    blocks, columns = counts.shape
    depth = 2 * acquisitions
    pixels = chosen_ref.shape[1]
    entries = list_ref.shape[1]
    per_block = entries // (blocks * columns)
    lane = lax.broadcasted_iota(jnp.int32, (1, entries), 1)
    limit = jnp.zeros((1, entries), jnp.int32)
    for a in range(blocks):
        for r in range(columns):
            start = (a * columns + r) * per_block
            inside = (lane >= start) & (lane < start + per_block)
            limit = jnp.where(inside, counts[a, r] + start, limit)
    listed = jnp.where(lane < limit, list_ref[...], -1)
    hits = lax.broadcasted_iota(jnp.int32, (pixels, entries), 0) == listed
    chosen = jnp.transpose(jnp.where(hits, 1.0, 0.0).astype(F32))
    chosen_ref[...] = chosen.astype(BF16)
    for a in range(blocks):
        for r in range(columns):
            start = (a * columns + r) * per_block
            covered = jnp.sum(chosen[start : start + per_block], axis=0, keepdims=True)
            clear_ref[a * columns + r] = jnp.broadcast_to(1.0 - covered, clear_ref.shape[1:])
    row = lax.broadcasted_iota(jnp.int32, (columns * depth, depth), 0)
    column_at = lax.broadcasted_iota(jnp.int32, (columns * depth, depth), 1)
    for r in range(columns):
        g = groups[r]
        pair = row // columns
        acq = pair % acq_share
        half = (pair // acq_share) % 2
        source = pair // (2 * acq_share)
        target = half * acquisitions + source * acq_share + acq
        hit = (column_at == target) & (row % columns == r)
        select = jnp.where(hit, 1.0, 0.0).astype(BF16)
        select_ref[r] = select
        real = steer_ref[g, 0]
        imag = steer_ref[g, 1]
        operator = jnp.concatenate(
            [
                jnp.concatenate([real, -imag], axis=1),
                jnp.concatenate([imag, real], axis=1),
            ],
            axis=0,
        )
        half_op_ref[r] = operator * jnp.asarray(STEP_SIZE, BF16)
        op_t = jnp.transpose(operator.astype(F32)).astype(BF16)
        op_t_ref[r] = op_t
        fmat_ref[:acquisitions, :acquisitions] = filter_ref[g, 0].astype(F32)
        fmat_ref[:acquisitions, acquisitions:] = -filter_ref[g, 1].astype(F32)
        fmat_ref[acquisitions:, :acquisitions] = filter_ref[g, 1].astype(F32)
        fmat_ref[acquisitions:, acquisitions:] = filter_ref[g, 0].astype(F32)
        beam = dot(op_t, fmat_ref[...].astype(BF16)).astype(BF16)
        wiener_ref[r] = dot(beam, select, (1, 1)).astype(BF16)


def profile_body(
    gather, half_op_ref, op_t_ref, wiener_ref, select_ref, chosen_ref, clear_ref,
    out_ref, grid_ref, real_ref, imag_ref, rounded_ref, target_ref, image_ref, sem,
):
    blocks, columns, elevation, pixels = out_ref.shape
    depth = op_t_ref.shape[2]
    per_block = chosen_ref.shape[0] // (blocks * columns)
    gather(grid_ref)
    picked = [
        dot(
            chosen_ref[a * columns * per_block : (a + 1) * columns * per_block],
            grid_ref[a],
            (1, 1),
        ).astype(BF16)
        for a in range(blocks)
    ]
    for r in range(columns):
        rows = jnp.concatenate(
            [p[r * per_block : (r + 1) * per_block] for p in picked], axis=0
        )
        target_ref[r] = dot(rows, select_ref[r])

    tile = 256

    def shrink(zr, zi):
        magnitude = zr * zr + zi * zi
        factor = jnp.maximum(
            1.0 - SHRINK * lax.rsqrt(jnp.maximum(magnitude, SHRINK * SHRINK)), 0.0
        )
        return zr * factor, zi * factor

    def update(r, misfit, first):
        for at in range(0, elevation, tile):
            zr = dot(misfit, half_op_ref[r, :, at : at + tile])
            zi = dot(misfit, half_op_ref[r, :, elevation + at : elevation + at + tile])
            if not first:
                zr = zr + real_ref[r, :, at : at + tile]
                zi = zi + imag_ref[r, :, at : at + tile]
            xr, xi = shrink(zr, zi)
            real_ref[r, :, at : at + tile] = xr
            imag_ref[r, :, at : at + tile] = xi
            rounded_ref[r, :, at : at + tile] = xr.astype(BF16)
            rounded_ref[r, :, elevation + at : elevation + at + tile] = xi.astype(BF16)

    for r in range(columns):
        update(r, target_ref[r].astype(BF16), True)

    def sweep(_, carry):
        for r in range(columns):
            misfit = (target_ref[r] - dot(rounded_ref[r], op_t_ref[r])).astype(BF16)
            update(r, misfit, False)
        return carry

    lax.fori_loop(0, ITERS - 1, sweep, 0)

    chunk = 128
    for a in range(blocks):
        for r in range(columns):
            clear = clear_ref[a * columns + r, :1]
            start = (a * columns + r) * per_block
            chosen = chosen_ref[start : start + per_block]
            for at in range(0, elevation, chunk):
                br = dot(wiener_ref[r, at : at + chunk], grid_ref[a])
                bi = dot(wiener_ref[r, elevation + at : elevation + at + chunk], grid_ref[a])
                xr = real_ref[r, a * per_block : (a + 1) * per_block, at : at + chunk]
                xi = imag_ref[r, a * per_block : (a + 1) * per_block, at : at + chunk]
                strength = (xr * xr + xi * xi).astype(BF16)
                placed = dot(strength, chosen, (0, 0))
                power = (br * br + bi * bi) * clear + placed
                image_ref[a, r, at : at + chunk] = power.astype(BF16)
            pltpu.make_async_copy(image_ref.at[a, r], out_ref.at[a, r], sem).start()
    for a in range(blocks):
        for r in range(columns):
            pltpu.make_async_copy(image_ref.at[a, r], out_ref.at[a, r], sem).wait()


def chunk_kernel(where, *refs):
    pieces = refs[:-15 + 1]
    rest = refs[-15 + 1 :]
    partners = len(pieces) - 1
    blocks = pieces[-1].shape[1]

    def gather(grid_ref):
        own = where[2 * partners]
        for d in range(partners):
            for j in range(2):
                at = where[2 * d + j]
                for a in range(blocks):
                    for half in range(2):
                        for t in range(grid_ref.shape[2] // LANES):
                            if j == 0:
                                part = pieces[d][own * blocks + a, half, t]
                            else:
                                part = pieces[-1][d, a, half, t]
                            size = part.shape[0]
                            first = pl.multiple_of(at * (2 * size) + half * size, size)
                            grid_ref[a, pl.ds(first, size), t * LANES : (t + 1) * LANES] = part

    profile_body(gather, *rest)


def plain_kernel(pieces, *rest):
    def gather(grid_ref):
        grid_ref[...] = pieces[...]

    profile_body(gather, *rest)


def shards(image_stack, steering, wiener_filter, range_group, lay_list, lay_count):
    halves, acq_share, azb_all, columns, pixels = image_stack.shape
    blocks = lay_list.shape[0]
    group_count, _, acquisitions, elevation = steering.shape
    depth = 2 * acquisitions
    chips = lax.axis_size("az")
    cores = lax.axis_size("acq")
    per_block = lay_list.shape[2]
    rows = blocks * per_block
    tiles = pixels // LANES
    chip = lax.axis_index("az")
    core = lax.axis_index("acq")
    pairwise = acq_share * columns == 16 and cores == 2 and chips & (chips - 1) == 0
    if pairwise:
        view = image_stack.reshape(halves, acq_share, azb_all, columns, tiles, LANES)
        view = view.transpose(0, 1, 2, 4, 3, 5)
        coords = jnp.stack([chip ^ d for d in range(chips)]).astype(jnp.int32)
        piece = jax.ShapeDtypeStruct(
            (cores * blocks, halves, tiles, acq_share, columns, LANES), BF16
        )
        chunks = pl.pallas_call(
            relay_kernel,
            out_shape=[piece] * chips,
            in_specs=[SMEM, ANY],
            out_specs=[VMEM] * chips,
            scratch_shapes=[pltpu.SemaphoreType.DMA],
            name="relay",
        )(coords, view)
        got = [chunks[0]] + [None] * (chips - 1)
        for d in [2, 3, 1] if chips == 4 else range(1, chips):
            got[d] = lax.ppermute(chunks[d], "az", [(i, i ^ d) for i in range(chips)])
        passing = jnp.stack(
            [lax.dynamic_slice_in_dim(g, (1 - core) * blocks, blocks, 0) for g in got]
        )
        passed = lax.ppermute(passing, "acq", [(0, 1), (1, 0)])
        flat = (halves, tiles, acq_share * columns, LANES)
        pieces = [g.reshape((cores * blocks,) + flat) for g in got]
        pieces.append(passed.reshape((chips, blocks) + flat))
        where = []
        for d in range(chips):
            where += [(chip ^ d) * 2 + core, (chip ^ d) * 2 + 1 - core]
        where = jnp.stack(where + [core]).astype(jnp.int32)
        lead = [where] + pieces
        body, lead_specs = chunk_kernel, [SMEM] + [VMEM] * len(pieces)
    else:
        moved = lax.all_to_all(
            image_stack, ("az", "acq"), split_axis=2, concat_axis=0, tiled=True
        )
        moved = moved.reshape(-1, acq_share, blocks, columns, pixels)
        lead = [moved.transpose(2, 0, 1, 3, 4).reshape(blocks, columns * depth, pixels)]
        body, lead_specs = plain_kernel, [VMEM]

    groups = (range_group - lax.axis_index("rg") * group_count).astype(jnp.int32)
    prepared = pl.pallas_call(
        lambda *refs: prepare_kernel(acq_share, *refs),
        out_shape=[
            jax.ShapeDtypeStruct((columns, depth, 2 * elevation), BF16),
            jax.ShapeDtypeStruct((columns, 2 * elevation, depth), BF16),
            jax.ShapeDtypeStruct((columns, 2 * elevation, columns * depth), BF16),
            jax.ShapeDtypeStruct((columns, columns * depth, depth), BF16),
            jax.ShapeDtypeStruct((blocks * columns * per_block, pixels), BF16),
            jax.ShapeDtypeStruct((blocks * columns, 8, pixels), F32),
        ],
        in_specs=[SMEM, SMEM, VMEM, VMEM, VMEM],
        out_specs=[VMEM] * 6,
        scratch_shapes=[pltpu.VMEM((depth, depth), F32)],
        cost_estimate=pl.CostEstimate(
            flops=1_000_000_000, bytes_accessed=4_000_000, transcendentals=0
        ),
        compiler_params=pltpu.CompilerParams(vmem_limit_bytes=16 << 20),
        name="prepare",
    )(groups, lay_count, lay_list.reshape(1, -1), steering, wiener_filter)

    return pl.pallas_call(
        body,
        out_shape=jax.ShapeDtypeStruct((blocks, columns, elevation, pixels), BF16),
        in_specs=lead_specs + [VMEM] * 6,
        out_specs=ANY,
        scratch_shapes=[
            pltpu.VMEM((blocks, columns * depth, pixels), BF16),
            pltpu.VMEM((columns, rows, elevation), F32),
            pltpu.VMEM((columns, rows, elevation), F32),
            pltpu.VMEM((columns, rows, 2 * elevation), BF16),
            pltpu.VMEM((columns, rows, depth), F32),
            pltpu.VMEM((blocks, columns, elevation, pixels), BF16),
            pltpu.SemaphoreType.DMA,
        ],
        compiler_params=pltpu.CompilerParams(vmem_limit_bytes=24 << 20),
        cost_estimate=pl.CostEstimate(
            flops=2_000_000_000, bytes_accessed=4_000_000, transcendentals=0
        ),
        name="profiles",
    )(*lead, *prepared)


def solution(mesh):
    return jax.shard_map(
        shards,
        mesh=mesh,
        in_specs=(
            P(None, ("az", "acq"), "groups", "rg", None),
            P("rg", None, None, None),
            P("rg", None, None, None),
            P("rg"),
            P(("groups", "az", "acq"), "rg", None),
            P(("groups", "az", "acq"), "rg"),
        ),
        out_specs=P(("groups", "az", "acq"), "rg", None, None),
        check_vma=False,
    )
```

```python
import jax
import jax.numpy as jnp
from jax import lax
from jax.experimental import pallas as pl
from jax.experimental.pallas import tpu as pltpu
from jax.sharding import PartitionSpec as P

ITERS = 8
STEP_SIZE = 0.5
SHRINK = 0.25
LANES = 128
WIENER_ROWS = 128
F32 = jnp.float32
BF16 = jnp.bfloat16

VMEM = pl.BlockSpec(memory_space=pltpu.VMEM)
SMEM = pl.BlockSpec(memory_space=pltpu.SMEM)
ANY = pl.BlockSpec(memory_space=pl.ANY)


def dot(a, b, contract=(1, 0)):
    return lax.dot_general(
        a, b, (((contract[0],), (contract[1],)), ((), ())), preferred_element_type=F32
    )


def relay_kernel(x_ref, *refs):
    chunks, sem = refs[:-1], refs[-1]
    halves, acq_share = x_ref.shape[:2]
    per_chip = chunks[0].shape[0]
    chip = lax.axis_index("az")
    copies = []
    for d, chunk in enumerate(chunks):
        first = (chip ^ d) * per_chip
        for half in range(halves):
            for acq in range(acq_share):
                copies.append(
                    pltpu.make_async_copy(
                        x_ref.at[half, acq, pl.ds(first, per_chip)],
                        chunk.at[:, half, :, acq],
                        sem,
                    )
                )
    for copy in copies:
        copy.start()
    for copy in copies:
        copy.wait()


def prepare_kernel(
    acq_share, groups, counts, list_ref, steer_ref, filter_ref,
    half_op_ref, op_t_ref, wiener_ref, select_ref, chosen_ref, clear_ref, fmat_ref,
):
    acquisitions, elevation = steer_ref.shape[2:]
    blocks, columns = counts.shape
    depth = 2 * acquisitions
    pixels = chosen_ref.shape[1]
    entries = list_ref.shape[1]
    per_block = entries // (blocks * columns)
    lane = lax.broadcasted_iota(jnp.int32, (1, entries), 1)
    limit = jnp.zeros((1, entries), jnp.int32)
    for a in range(blocks):
        for r in range(columns):
            start = (a * columns + r) * per_block
            inside = (lane >= start) & (lane < start + per_block)
            limit = jnp.where(inside, counts[a, r] + start, limit)
    listed = jnp.where(lane < limit, list_ref[...], -1)
    hits = lax.broadcasted_iota(jnp.int32, (pixels, entries), 0) == listed
    chosen = jnp.transpose(jnp.where(hits, 1.0, 0.0).astype(F32))
    chosen_ref[...] = chosen.astype(BF16)
    for a in range(blocks):
        for r in range(columns):
            start = (a * columns + r) * per_block
            covered = jnp.sum(chosen[start : start + per_block], axis=0, keepdims=True)
            clear_ref[a * columns + r] = jnp.broadcast_to(1.0 - covered, clear_ref.shape[1:])
    row = lax.broadcasted_iota(jnp.int32, (columns * depth, depth), 0)
    column_at = lax.broadcasted_iota(jnp.int32, (columns * depth, depth), 1)
    for r in range(columns):
        g = groups[r] - lax.axis_index("rg") * steer_ref.shape[0]
        pair = row // columns
        acq = pair % acq_share
        half = (pair // acq_share) % 2
        source = pair // (2 * acq_share)
        target = half * acquisitions + source * acq_share + acq
        hit = (column_at == target) & (row % columns == r)
        select = jnp.where(hit, 1.0, 0.0).astype(BF16)
        select_ref[r] = select
        real = steer_ref[g, 0]
        imag = steer_ref[g, 1]
        operator = jnp.concatenate(
            [
                jnp.concatenate([real, -imag], axis=1),
                jnp.concatenate([imag, real], axis=1),
            ],
            axis=0,
        )
        half_op_ref[r] = operator * jnp.asarray(STEP_SIZE, BF16)
        op_t = jnp.transpose(operator.astype(F32)).astype(BF16)
        op_t_ref[r] = op_t
        fmat_ref[:acquisitions, :acquisitions] = filter_ref[g, 0].astype(F32)
        fmat_ref[:acquisitions, acquisitions:] = -filter_ref[g, 1].astype(F32)
        fmat_ref[acquisitions:, :acquisitions] = filter_ref[g, 1].astype(F32)
        fmat_ref[acquisitions:, acquisitions:] = filter_ref[g, 0].astype(F32)
        beam = dot(op_t, fmat_ref[...].astype(BF16)).astype(BF16)
        wiener_ref[r] = dot(beam, select, (1, 1)).astype(BF16)


def profile_body(
    gather, half_op_ref, op_t_ref, wiener_ref, select_ref, chosen_ref, clear_ref,
    out_ref, grid_ref, real_ref, imag_ref, rounded_ref, target_ref, image_ref, sem,
):
    blocks, columns, elevation, pixels = out_ref.shape
    per_block = chosen_ref.shape[0] // (blocks * columns)
    gather(grid_ref)
    picked = [
        dot(
            chosen_ref[a * columns * per_block : (a + 1) * columns * per_block],
            grid_ref[a],
            (1, 1),
        ).astype(BF16)
        for a in range(blocks)
    ]
    for r in range(columns):
        rows = jnp.concatenate(
            [p[r * per_block : (r + 1) * per_block] for p in picked], axis=0
        )
        target_ref[r] = dot(rows, select_ref[r])

    tile = 256

    def update(r, misfit, first):
        for at in range(0, elevation, tile):
            zr = dot(misfit, half_op_ref[r, :, at : at + tile])
            zi = dot(misfit, half_op_ref[r, :, elevation + at : elevation + at + tile])
            if not first:
                zr = zr + real_ref[r, :, at : at + tile]
                zi = zi + imag_ref[r, :, at : at + tile]
            magnitude = zr * zr + zi * zi
            factor = jnp.maximum(
                1.0 - SHRINK * lax.rsqrt(jnp.maximum(magnitude, SHRINK * SHRINK)), 0.0
            )
            xr = zr * factor
            xi = zi * factor
            real_ref[r, :, at : at + tile] = xr
            imag_ref[r, :, at : at + tile] = xi
            rounded_ref[r, :, at : at + tile] = xr.astype(BF16)
            rounded_ref[r, :, elevation + at : elevation + at + tile] = xi.astype(BF16)

    shares = [(a, r, at) for a in range(blocks) for at in range(0, elevation, WIENER_ROWS)
              for r in range(columns)]

    def wiener(a, r, at):
        br = dot(wiener_ref[r, at : at + WIENER_ROWS], grid_ref[a])
        bi = dot(wiener_ref[r, elevation + at : elevation + at + WIENER_ROWS], grid_ref[a])
        power = (br * br + bi * bi) * clear_ref[a * columns + r, :1]
        image_ref[a, r, at : at + WIENER_ROWS] = power.astype(BF16)

    done = 0
    for t in range(ITERS):
        for r in range(columns):
            if t == 0:
                misfit = target_ref[r].astype(BF16)
            else:
                misfit = (target_ref[r] - dot(rounded_ref[r], op_t_ref[r])).astype(BF16)
            update(r, misfit, t == 0)
        until = len(shares) * (t + 1) // ITERS
        for share in shares[done:until]:
            wiener(*share)
        done = until

    for r in range(columns):
        for a in range(blocks):
            start = (a * columns + r) * per_block
            chosen = chosen_ref[start : start + per_block]
            xr = real_ref[r, a * per_block : (a + 1) * per_block]
            xi = imag_ref[r, a * per_block : (a + 1) * per_block]
            strength = (xr * xr + xi * xi).astype(BF16)
            placed = dot(strength, chosen, (0, 0)).astype(BF16)
            image_ref[a, r] = image_ref[a, r] + placed
            pltpu.make_async_copy(image_ref.at[a, r], out_ref.at[a, r], sem).start()
    for a in range(blocks):
        for r in range(columns):
            pltpu.make_async_copy(image_ref.at[a, r], out_ref.at[a, r], sem).wait()


def chunk_kernel(*refs):
    pieces, rest = refs[:-14], refs[-14:]
    partners = len(pieces) - 1
    blocks = pieces[-1].shape[1]

    def gather(grid_ref):
        chip, core = lax.axis_index("az"), lax.axis_index("acq")
        for d in range(partners):
            for j in range(2):
                at = (chip ^ d) * 2 + (core ^ j)
                for a in range(blocks):
                    for half in range(2):
                        for t in range(grid_ref.shape[2] // LANES):
                            if j == 0:
                                part = pieces[d][core * blocks + a, half, t]
                            else:
                                part = pieces[-1][d, a, half, t]
                            size = part.shape[0]
                            first = pl.multiple_of(at * (2 * size) + half * size, size)
                            grid_ref[a, pl.ds(first, size), t * LANES : (t + 1) * LANES] = part

    profile_body(gather, *rest)


def plain_kernel(pieces, *rest):
    def gather(grid_ref):
        grid_ref[...] = pieces[...]

    profile_body(gather, *rest)


def shards(image_stack, steering, wiener_filter, range_group, lay_list, lay_count):
    halves, acq_share, azb_all, columns, pixels = image_stack.shape
    blocks = lay_list.shape[0]
    group_count, _, acquisitions, elevation = steering.shape
    depth = 2 * acquisitions
    chips = lax.axis_size("az")
    cores = lax.axis_size("acq")
    per_block = lay_list.shape[2]
    rows = blocks * per_block
    tiles = pixels // LANES
    chip = lax.axis_index("az")
    core = lax.axis_index("acq")
    pairwise = acq_share * columns == 16 and cores == 2 and chips & (chips - 1) == 0
    prepared = pl.pallas_call(
        lambda *refs: prepare_kernel(acq_share, *refs),
        out_shape=[
            jax.ShapeDtypeStruct((columns, depth, 2 * elevation), BF16),
            jax.ShapeDtypeStruct((columns, 2 * elevation, depth), BF16),
            jax.ShapeDtypeStruct((columns, 2 * elevation, columns * depth), BF16),
            jax.ShapeDtypeStruct((columns, columns * depth, depth), BF16),
            jax.ShapeDtypeStruct((blocks * columns * per_block, pixels), BF16),
            jax.ShapeDtypeStruct((blocks * columns, 8, pixels), F32),
        ],
        in_specs=[SMEM, SMEM, VMEM, VMEM, VMEM],
        out_specs=[VMEM] * 6,
        scratch_shapes=[pltpu.VMEM((depth, depth), F32)],
        cost_estimate=pl.CostEstimate(
            flops=1_000_000_000, bytes_accessed=4_000_000, transcendentals=0
        ),
        compiler_params=pltpu.CompilerParams(vmem_limit_bytes=16 << 20),
        name="prepare",
    )(range_group, lay_count, lay_list.reshape(1, -1), steering, wiener_filter)

    if pairwise:
        view = image_stack.reshape(halves, acq_share, azb_all, columns, tiles, LANES)
        view = view.transpose(0, 1, 2, 4, 3, 5)
        piece = jax.ShapeDtypeStruct(
            (cores * blocks, halves, tiles, acq_share, columns, LANES), BF16
        )
        chunks = pl.pallas_call(
            relay_kernel,
            out_shape=[piece] * chips,
            in_specs=[ANY],
            out_specs=[VMEM] * chips,
            scratch_shapes=[pltpu.SemaphoreType.DMA],
            compiler_params=pltpu.CompilerParams(vmem_limit_bytes=2 << 20),
            name="relay",
        )(view)
        got = [chunks[0]] + [None] * (chips - 1)
        for d in range(1, chips):
            with jax.named_scope(f"swap{d}"):
                got[d] = lax.ppermute(chunks[d], "az", [(i, i ^ d) for i in range(chips)])
        passing = jnp.stack(
            [lax.dynamic_slice_in_dim(g, (1 - core) * blocks, blocks, 0) for g in got]
        )
        passing, prepared = lax.optimization_barrier((passing, prepared))
        passed = lax.ppermute(passing, "acq", [(0, 1), (1, 0)])
        flat = (halves, tiles, acq_share * columns, LANES)
        pieces = [g.reshape((cores * blocks,) + flat) for g in got]
        pieces.append(passed.reshape((chips, blocks) + flat))
        lead = pieces
        body, lead_specs = chunk_kernel, [VMEM] * len(pieces)
    else:
        moved = lax.all_to_all(
            image_stack, ("az", "acq"), split_axis=2, concat_axis=0, tiled=True
        )
        moved = moved.reshape(-1, acq_share, blocks, columns, pixels)
        lead = [moved.transpose(2, 0, 1, 3, 4).reshape(blocks, columns * depth, pixels)]
        body, lead_specs = plain_kernel, [VMEM]

    return pl.pallas_call(
        body,
        out_shape=jax.ShapeDtypeStruct((blocks, columns, elevation, pixels), BF16),
        in_specs=lead_specs + [VMEM] * 6,
        out_specs=ANY,
        scratch_shapes=[
            pltpu.VMEM((blocks, columns * depth, pixels), BF16),
            pltpu.VMEM((columns, rows, elevation), F32),
            pltpu.VMEM((columns, rows, elevation), F32),
            pltpu.VMEM((columns, rows, 2 * elevation), BF16),
            pltpu.VMEM((columns, rows, depth), F32),
            pltpu.VMEM((blocks, columns, elevation, pixels), BF16),
            pltpu.SemaphoreType.DMA,
        ],
        compiler_params=pltpu.CompilerParams(vmem_limit_bytes=24 << 20),
        cost_estimate=pl.CostEstimate(
            flops=2_000_000_000, bytes_accessed=4_000_000, transcendentals=0
        ),
        name="profiles",
    )(*lead, *prepared)


def solution(mesh):
    return jax.shard_map(
        shards,
        mesh=mesh,
        in_specs=(
            P(None, ("az", "acq"), "groups", "rg", None),
            P("rg", None, None, None),
            P("rg", None, None, None),
            P("rg"),
            P(("groups", "az", "acq"), "rg", None),
            P(("groups", "az", "acq"), "rg"),
        ),
        out_specs=P(("groups", "az", "acq"), "rg", None, None),
        check_vma=False,
    )
```

```python
import jax
import jax.numpy as jnp
from jax import lax
from jax.experimental import pallas as pl
from jax.experimental.pallas import tpu as pltpu
from jax.sharding import PartitionSpec as P

ITERS = 8
STEP_SIZE = 0.5
SHRINK = 0.25
LANES = 128
WIENER_ROWS = 128
F32 = jnp.float32
BF16 = jnp.bfloat16

VMEM = pl.BlockSpec(memory_space=pltpu.VMEM)
SMEM = pl.BlockSpec(memory_space=pltpu.SMEM)
ANY = pl.BlockSpec(memory_space=pl.ANY)


def dot(a, b, contract=(1, 0)):
    return lax.dot_general(
        a, b, (((contract[0],), (contract[1],)), ((), ())), preferred_element_type=F32
    )


def relay_kernel(places, x_ref, *refs):
    chunks, sem = refs[:-1], refs[-1]
    halves, acq_share = x_ref.shape[:2]
    chip, core = lax.axis_index("az"), lax.axis_index("acq")
    cores = lax.axis_size("acq")
    copies = []
    for owners, chunk in zip(places, chunks):
        blocks = chunk.shape[0] // len(owners)
        for at, (d, j) in enumerate(owners):
            first = ((chip ^ d) * cores + (core ^ j)) * blocks
            for half in range(halves):
                for acq in range(acq_share):
                    copies.append(
                        pltpu.make_async_copy(
                            x_ref.at[half, acq, pl.ds(first, blocks)],
                            chunk.at[pl.ds(at * blocks, blocks), half, :, acq],
                            sem,
                        )
                    )
    for copy in copies:
        copy.start()
    for copy in copies:
        copy.wait()


def prepare_kernel(
    acq_share, relative, groups, counts, list_ref, steer_ref, filter_ref,
    first_ref, half_op_ref, op_t_ref, wiener_ref, select_ref, chosen_ref, clear_ref, fmat_ref,
):
    acquisitions, _ = steer_ref.shape[2:]
    blocks, columns = counts.shape
    depth = 2 * acquisitions
    pixels = chosen_ref.shape[1]
    entries = list_ref.shape[1]
    per_block = entries // (blocks * columns)
    lane = lax.broadcasted_iota(jnp.int32, (1, entries), 1)
    limit = jnp.zeros((1, entries), jnp.int32)
    for a in range(blocks):
        for r in range(columns):
            start = (a * columns + r) * per_block
            inside = (lane >= start) & (lane < start + per_block)
            limit = jnp.where(inside, counts[a, r] + start, limit)
    listed = jnp.where(lane < limit, list_ref[...], -1)
    hits = lax.broadcasted_iota(jnp.int32, (pixels, entries), 0) == listed
    chosen = jnp.transpose(jnp.where(hits, 1.0, 0.0).astype(F32))
    chosen_ref[...] = chosen.astype(BF16)
    for a in range(blocks):
        for r in range(columns):
            start = (a * columns + r) * per_block
            covered = jnp.sum(chosen[start : start + per_block], axis=0, keepdims=True)
            clear_ref[a * columns + r] = jnp.broadcast_to(1.0 - covered, clear_ref.shape[1:])
    row = lax.broadcasted_iota(jnp.int32, (columns * depth, depth), 0)
    column_at = lax.broadcasted_iota(jnp.int32, (columns * depth, depth), 1)
    for r in range(columns):
        g = groups[r] - lax.axis_index("rg") * steer_ref.shape[0]
        pair = row // columns
        acq = pair % acq_share
        half = (pair // acq_share) % 2
        source = pair // (2 * acq_share)
        if relative:
            cores = lax.axis_size("acq")
            chip, core = lax.axis_index("az"), lax.axis_index("acq")
            source = ((source // cores) ^ chip) * cores + ((source % cores) ^ core)
        target = half * acquisitions + source * acq_share + acq
        hit = (column_at == target) & (row % columns == r)
        select = jnp.where(hit, 1.0, 0.0).astype(BF16)
        select_ref[r] = select
        real = steer_ref[g, 0]
        imag = steer_ref[g, 1]
        operator = jnp.concatenate(
            [
                jnp.concatenate([real, -imag], axis=1),
                jnp.concatenate([imag, real], axis=1),
            ],
            axis=0,
        )
        half_op = operator * jnp.asarray(STEP_SIZE, BF16)
        half_op_ref[r] = half_op
        first_ref[r] = dot(select, half_op).astype(BF16)
        op_t = jnp.transpose(operator.astype(F32)).astype(BF16)
        op_t_ref[r] = op_t
        fmat_ref[:acquisitions, :acquisitions] = filter_ref[g, 0].astype(F32)
        fmat_ref[:acquisitions, acquisitions:] = -filter_ref[g, 1].astype(F32)
        fmat_ref[acquisitions:, :acquisitions] = filter_ref[g, 1].astype(F32)
        fmat_ref[acquisitions:, acquisitions:] = filter_ref[g, 0].astype(F32)
        beam = dot(op_t, fmat_ref[...].astype(BF16)).astype(BF16)
        wiener_ref[r] = dot(beam, select, (1, 1)).astype(BF16)


def profile_body(
    grid, first_ref, half_op_ref, op_t_ref, wiener_ref, select_ref, chosen_ref, clear_ref,
    out_ref, real_ref, imag_ref, rounded_ref, target_ref, image_ref, sem,
):
    blocks, columns, elevation, _ = out_ref.shape
    per_block = chosen_ref.shape[0] // (blocks * columns)
    picked = [
        dot(
            chosen_ref[a * columns * per_block : (a + 1) * columns * per_block],
            grid(a),
            (1, 1),
        ).astype(BF16)
        for a in range(blocks)
    ]
    picked = [
        jnp.concatenate([p[r * per_block : (r + 1) * per_block] for p in picked], axis=0)
        for r in range(columns)
    ]
    for r in range(columns):
        target_ref[r] = dot(picked[r], select_ref[r])

    tile = 256

    def update(r, misfit, op_ref, first):
        for at in range(0, elevation, tile):
            zr = dot(misfit, op_ref[r, :, at : at + tile])
            zi = dot(misfit, op_ref[r, :, elevation + at : elevation + at + tile])
            if not first:
                zr = zr + real_ref[r, :, at : at + tile]
                zi = zi + imag_ref[r, :, at : at + tile]
            magnitude = zr * zr + zi * zi
            factor = jnp.maximum(
                1.0 - SHRINK * lax.rsqrt(jnp.maximum(magnitude, SHRINK * SHRINK)), 0.0
            )
            xr = zr * factor
            xi = zi * factor
            real_ref[r, :, at : at + tile] = xr
            imag_ref[r, :, at : at + tile] = xi
            rounded_ref[r, :, at : at + tile] = xr.astype(BF16)
            rounded_ref[r, :, elevation + at : elevation + at + tile] = xi.astype(BF16)

    shares = [(a, r, at) for a in range(blocks) for at in range(0, elevation, WIENER_ROWS)
              for r in range(columns)]

    def wiener(a, r, at):
        br = dot(wiener_ref[r, at : at + WIENER_ROWS], grid(a))
        bi = dot(wiener_ref[r, elevation + at : elevation + at + WIENER_ROWS], grid(a))
        power = (br * br + bi * bi) * clear_ref[a * columns + r, :1]
        image_ref[a, r, at : at + WIENER_ROWS] = power.astype(BF16)

    done = 0
    for t in range(ITERS):
        for r in range(columns):
            if t == 0:
                update(r, picked[r], first_ref, True)
            else:
                misfit = (target_ref[r] - dot(rounded_ref[r], op_t_ref[r])).astype(BF16)
                update(r, misfit, half_op_ref, False)
        until = len(shares) * (t + 1) // ITERS
        for share in shares[done:until]:
            wiener(*share)
        done = until

    for r in range(columns):
        for a in range(blocks):
            start = (a * columns + r) * per_block
            chosen = chosen_ref[start : start + per_block]
            xr = real_ref[r, a * per_block : (a + 1) * per_block]
            xi = imag_ref[r, a * per_block : (a + 1) * per_block]
            strength = (xr * xr + xi * xi).astype(BF16)
            placed = dot(strength, chosen, (0, 0)).astype(BF16)
            image_ref[a, r] = image_ref[a, r] + placed
            pltpu.make_async_copy(image_ref.at[a, r], out_ref.at[a, r], sem).start()
    for a in range(blocks):
        for r in range(columns):
            pltpu.make_async_copy(image_ref.at[a, r], out_ref.at[a, r], sem).wait()


def join_kernel(skips, *refs):
    out_ref = refs[-1]
    at = 0
    for skip, ref in zip(skips, refs[:-1]):
        size = ref.shape[0] - skip
        out_ref[at : at + size] = ref[skip:]
        at += size


def pieces_kernel(count, order, *refs):
    pieces, rest = refs[:count], refs[count:]

    def grid(a):
        rows = []
        for at, lead in order:
            ref = pieces[at]
            where = lead + (a,) if len(ref.shape) == 6 else (a,)
            halves, tiles = ref.shape[-4:-2]
            for half in range(halves):
                rows.append(
                    jnp.concatenate(
                        [ref[where + (half, t)] for t in range(tiles)], axis=1
                    )
                )
        return jnp.concatenate(rows, axis=0)

    profile_body(grid, *rest)


def plain_kernel(pieces, *rest):
    profile_body(lambda a: pieces[a], *rest)


def shards(image_stack, steering, wiener_filter, range_group, lay_list, lay_count):
    halves, acq_share, azb_all, columns, pixels = image_stack.shape
    blocks = lay_list.shape[0]
    _, _, acquisitions, elevation = steering.shape
    depth = 2 * acquisitions
    chips = lax.axis_size("az")
    cores = lax.axis_size("acq")
    per_block = lay_list.shape[2]
    rows = blocks * per_block
    tiles = pixels // LANES
    pairwise = acq_share * columns == 16 and cores == 2 and chips & (chips - 1) == 0
    prepared = pl.pallas_call(
        lambda *refs: prepare_kernel(acq_share, pairwise, *refs),
        out_shape=[
            jax.ShapeDtypeStruct((columns, columns * depth, 2 * elevation), BF16),
            jax.ShapeDtypeStruct((columns, depth, 2 * elevation), BF16),
            jax.ShapeDtypeStruct((columns, 2 * elevation, depth), BF16),
            jax.ShapeDtypeStruct((columns, 2 * elevation, columns * depth), BF16),
            jax.ShapeDtypeStruct((columns, columns * depth, depth), BF16),
            jax.ShapeDtypeStruct((blocks * columns * per_block, pixels), BF16),
            jax.ShapeDtypeStruct((blocks * columns, 8, pixels), F32),
        ],
        in_specs=[SMEM, SMEM, VMEM, VMEM, VMEM],
        out_specs=[VMEM] * 7,
        scratch_shapes=[pltpu.VMEM((depth, depth), F32)],
        cost_estimate=pl.CostEstimate(
            flops=1_000_000_000, bytes_accessed=4_000_000, transcendentals=0
        ),
        compiler_params=pltpu.CompilerParams(vmem_limit_bytes=16 << 20),
        name="prepare",
    )(range_group, lay_count, lay_list.reshape(1, -1), steering, wiener_filter)

    if pairwise:
        view = image_stack.reshape(halves, acq_share, azb_all, columns, tiles, LANES)
        view = view.transpose(0, 1, 2, 4, 3, 5)
        far = chips - 1
        turns = sorted(range(1, chips), key=lambda d: (d < chips // 2, d))
        places = [[(0, 0)], [(0, 1)]]
        for d in turns:
            places += [[(d, 0)], [(d, 1)]] if d == far else [[(d, 0), (d, 1)]]
        unit = (halves, tiles, acq_share, columns, LANES)
        chunks = pl.pallas_call(
            lambda *refs: relay_kernel(places, *refs),
            out_shape=[
                jax.ShapeDtypeStruct((len(owners) * blocks,) + unit, BF16)
                for owners in places
            ],
            in_specs=[ANY],
            out_specs=[VMEM] * len(places),
            scratch_shapes=[pltpu.SemaphoreType.DMA],
            compiler_params=pltpu.CompilerParams(vmem_limit_bytes=2 << 20),
            name="relay",
        )(view)
        flat = (halves, tiles, acq_share * columns, LANES)
        chunks = [chunk.reshape((-1,) + flat) for chunk in chunks]
        got, waiting = {(0, 0): chunks[0]}, [((0, 1), chunks[1])]
        for owners, chunk in zip(places[2:], chunks[2:]):
            d, j = owners[0]
            straight = [
                (c * cores + q, (c ^ d) * cores + (q ^ j))
                for c in range(chips)
                for q in range(cores)
            ]
            arrived = lax.ppermute(chunk, ("az", "acq"), straight)
            got[d, j] = arrived
            if len(owners) == 2:
                waiting.append(((d, 1), arrived))
        skips = [w.shape[0] - blocks for _, w in waiting]
        passing = pl.pallas_call(
            lambda *refs: join_kernel(skips, *refs),
            out_shape=jax.ShapeDtypeStruct((len(waiting) * blocks,) + flat, BF16),
            in_specs=[VMEM] * len(waiting),
            out_specs=VMEM,
            compiler_params=pltpu.CompilerParams(vmem_limit_bytes=2 << 20),
            name="join",
        )(*[w for _, w in waiting])
        passing, prepared = lax.optimization_barrier((passing, prepared))
        passed = lax.ppermute(passing, "acq", [(0, 1), (1, 0)])
        arrays, order = [], {}
        for place, array in got.items():
            order[place] = (len(arrays), ())
            arrays.append(array)
        for at, (place, _) in enumerate(waiting):
            order[place] = (len(arrays), (at,))
        arrays.append(passed.reshape((len(waiting), blocks) + flat))
        order = [order[d, j] for d in range(chips) for j in range(cores)]
        lead = arrays
        body = lambda *refs: pieces_kernel(len(arrays), order, *refs)
    else:
        moved = lax.all_to_all(
            image_stack, ("az", "acq"), split_axis=2, concat_axis=0, tiled=True
        )
        moved = moved.reshape(-1, acq_share, blocks, columns, pixels)
        lead = [moved.transpose(2, 0, 1, 3, 4).reshape(blocks, columns * depth, pixels)]
        body = plain_kernel

    return pl.pallas_call(
        body,
        out_shape=jax.ShapeDtypeStruct((blocks, columns, elevation, pixels), BF16),
        in_specs=[VMEM] * (len(lead) + len(prepared)),
        out_specs=ANY,
        scratch_shapes=[
            pltpu.VMEM((columns, rows, elevation), F32),
            pltpu.VMEM((columns, rows, elevation), F32),
            pltpu.VMEM((columns, rows, 2 * elevation), BF16),
            pltpu.VMEM((columns, rows, depth), F32),
            pltpu.VMEM((blocks, columns, elevation, pixels), BF16),
            pltpu.SemaphoreType.DMA,
        ],
        compiler_params=pltpu.CompilerParams(vmem_limit_bytes=24 << 20),
        cost_estimate=pl.CostEstimate(
            flops=2_000_000_000, bytes_accessed=4_000_000, transcendentals=0
        ),
        name="profiles",
    )(*lead, *prepared)


def solution(mesh):
    return jax.shard_map(
        shards,
        mesh=mesh,
        in_specs=(
            P(None, ("az", "acq"), "groups", "rg", None),
            P("rg", None, None, None),
            P("rg", None, None, None),
            P("rg"),
            P(("groups", "az", "acq"), "rg", None),
            P(("groups", "az", "acq"), "rg"),
        ),
        out_specs=P(("groups", "az", "acq"), "rg", None, None),
        check_vma=False,
    )
```

```python
import jax
import jax.numpy as jnp
from jax import lax
from jax.experimental import pallas as pl
from jax.experimental.pallas import tpu as pltpu
from jax.sharding import PartitionSpec as P

ITERS = 8
STEP_SIZE = 0.5
SHRINK = 0.25
LANES = 128
WIENER_ROWS = 128
F32 = jnp.float32
BF16 = jnp.bfloat16

VMEM = pl.BlockSpec(memory_space=pltpu.VMEM)
ANY = pl.BlockSpec(memory_space=pl.ANY)
HBM = pl.BlockSpec(memory_space=pltpu.HBM)


def dot(a, b, contract=(1, 0)):
    return lax.dot_general(
        a, b, (((contract[0],), (contract[1],)), ((), ())), preferred_element_type=F32
    )


def relay_kernel(places, extra, x_ref, *refs):
    inputs, refs = refs[:extra], refs[extra:]
    chunks, fetched = refs[: len(places)], refs[len(places) : len(places) + extra]
    stack_ref, stack_sem, sems = refs[len(places) + extra :]
    halves, acq_share, _, tiles = x_ref.shape[:4]
    whole = pltpu.make_async_copy(x_ref, stack_ref, stack_sem)
    whole.start()
    copies = [
        pltpu.make_async_copy(source, target, sems.at[at])
        for at, (source, target) in enumerate(zip(inputs, fetched))
    ]
    for copy in copies:
        copy.start()
    chip, core = lax.axis_index("az"), lax.axis_index("acq")
    cores = lax.axis_size("acq")
    whole.wait()
    for owners, chunk in zip(places, chunks):
        blocks = chunk.shape[0] // len(owners)
        for at, (d, j) in enumerate(owners):
            first = ((chip ^ d) * cores + (core ^ j)) * blocks
            for a in range(blocks):
                for half in range(halves):
                    for t in range(tiles):
                        for acq in range(acq_share):
                            chunk[at * blocks + a, half, t, acq] = stack_ref[
                                half, acq, first + a, t
                            ]
    for copy in copies:
        copy.wait()


def prepare_kernel(
    acq_share, relative, groups, counts, list_ref, steer_ref, filter_ref,
    first_ref, half_op_ref, op_t_ref, wiener_ref, select_ref, chosen_ref, clear_ref, fmat_ref,
):
    group_count, _, acquisitions, _ = steer_ref.shape
    blocks, columns, per_block = list_ref.shape
    depth = 2 * acquisitions
    pixels = chosen_ref.shape[1]
    first_group = lax.axis_index("rg") * group_count
    row = lax.broadcasted_iota(jnp.int32, (per_block, per_block), 0)
    lane = lax.broadcasted_iota(jnp.int32, (per_block, per_block), 1)
    entry = lax.broadcasted_iota(jnp.int32, (per_block, pixels), 0)
    pixel = lax.broadcasted_iota(jnp.int32, (per_block, pixels), 1)
    for a in range(blocks):
        for r in range(columns):
            listed = list_ref[a, r : r + 1].astype(F32)
            upright = jnp.sum(jnp.where(row == lane, listed, 0.0), axis=1, keepdims=True)
            usable = entry < counts[a : a + 1, r : r + 1]
            hit = (upright.astype(jnp.int32) == pixel) & usable
            chosen = jnp.where(hit, 1.0, 0.0).astype(F32)
            start = (a * columns + r) * per_block
            chosen_ref[start : start + per_block] = chosen.astype(BF16)
            covered = jnp.sum(chosen, axis=0, keepdims=True)
            clear_ref[a * columns + r] = jnp.broadcast_to(1.0 - covered, clear_ref.shape[1:])
    at = lax.broadcasted_iota(jnp.int32, (1, depth), 1)
    half, acq = at // acquisitions, at % acquisitions
    source = acq // acq_share
    if relative:
        cores = lax.axis_size("acq")
        chip, core = lax.axis_index("az"), lax.axis_index("acq")
        source = ((source // cores) ^ chip) * cores + ((source % cores) ^ core)
    place = ((source * 2 + half) * acq_share + acq % acq_share) * columns
    long = lax.broadcasted_iota(jnp.int32, (columns * depth, depth), 0)
    for r in range(columns):
        g = jnp.max(groups[:, r : r + 1]) - first_group
        select = jnp.where(long == place + r, 1.0, 0.0).astype(BF16)
        select_ref[r] = select
        real = steer_ref[g, 0]
        imag = steer_ref[g, 1]
        operator = jnp.concatenate(
            [
                jnp.concatenate([real, -imag], axis=1),
                jnp.concatenate([imag, real], axis=1),
            ],
            axis=0,
        )
        half_op = operator * jnp.asarray(STEP_SIZE, BF16)
        half_op_ref[r] = half_op
        first_ref[r] = dot(select, half_op).astype(BF16)
        op_t = jnp.transpose(operator.astype(F32)).astype(BF16)
        op_t_ref[r] = op_t
        fmat_ref[:acquisitions, :acquisitions] = filter_ref[g, 0].astype(F32)
        fmat_ref[:acquisitions, acquisitions:] = -filter_ref[g, 1].astype(F32)
        fmat_ref[acquisitions:, :acquisitions] = filter_ref[g, 1].astype(F32)
        fmat_ref[acquisitions:, acquisitions:] = filter_ref[g, 0].astype(F32)
        spread = dot(fmat_ref[...].astype(BF16), select, (1, 1)).astype(BF16)
        wiener_ref[r] = dot(op_t, spread).astype(BF16)


def profile_body(
    grid, first_ref, half_op_ref, op_t_ref, wiener_ref, select_ref, chosen_ref, clear_ref,
    out_ref, real_ref, imag_ref, rounded_ref, target_ref, image_ref, sem,
):
    blocks, columns, elevation, _ = out_ref.shape
    per_block = chosen_ref.shape[0] // (blocks * columns)
    picked = [
        dot(
            chosen_ref[a * columns * per_block : (a + 1) * columns * per_block],
            grid(a),
            (1, 1),
        ).astype(BF16)
        for a in range(blocks)
    ]
    picked = [
        jnp.concatenate([p[r * per_block : (r + 1) * per_block] for p in picked], axis=0)
        for r in range(columns)
    ]
    for r in range(columns):
        target_ref[r] = dot(picked[r], select_ref[r])

    tile = 256

    def update(r, misfit, op_ref, first):
        for at in range(0, elevation, tile):
            zr = dot(misfit, op_ref[r, :, at : at + tile])
            zi = dot(misfit, op_ref[r, :, elevation + at : elevation + at + tile])
            if not first:
                zr = zr + real_ref[r, :, at : at + tile]
                zi = zi + imag_ref[r, :, at : at + tile]
            magnitude = zr * zr + zi * zi
            factor = jnp.maximum(
                1.0 - SHRINK * lax.rsqrt(jnp.maximum(magnitude, SHRINK * SHRINK)), 0.0
            )
            xr = zr * factor
            xi = zi * factor
            real_ref[r, :, at : at + tile] = xr
            imag_ref[r, :, at : at + tile] = xi
            rounded_ref[r, :, at : at + tile] = xr.astype(BF16)
            rounded_ref[r, :, elevation + at : elevation + at + tile] = xi.astype(BF16)

    shares = [(a, r, at) for a in range(blocks) for at in range(0, elevation, WIENER_ROWS)
              for r in range(columns)]

    def wiener(a, r, at):
        br = dot(wiener_ref[r, at : at + WIENER_ROWS], grid(a))
        bi = dot(wiener_ref[r, elevation + at : elevation + at + WIENER_ROWS], grid(a))
        power = (br * br + bi * bi) * clear_ref[a * columns + r, :1]
        image_ref[a, r, at : at + WIENER_ROWS] = power.astype(BF16)

    done = 0
    for t in range(ITERS):
        for r in range(columns):
            if t == 0:
                update(r, picked[r], first_ref, True)
            else:
                misfit = (target_ref[r] - dot(rounded_ref[r], op_t_ref[r])).astype(BF16)
                update(r, misfit, half_op_ref, False)
        until = len(shares) * (t + 1) // ITERS
        for share in shares[done:until]:
            wiener(*share)
        done = until

    for r in range(columns):
        for a in range(blocks):
            start = (a * columns + r) * per_block
            chosen = chosen_ref[start : start + per_block]
            xr = real_ref[r, a * per_block : (a + 1) * per_block]
            xi = imag_ref[r, a * per_block : (a + 1) * per_block]
            strength = (xr * xr + xi * xi).astype(BF16)
            placed = dot(strength, chosen, (0, 0)).astype(BF16)
            image_ref[a, r] = image_ref[a, r] + placed
            pltpu.make_async_copy(image_ref.at[a, r], out_ref.at[a, r], sem).start()
    for a in range(blocks):
        for r in range(columns):
            pltpu.make_async_copy(image_ref.at[a, r], out_ref.at[a, r], sem).wait()


def join_kernel(skips, *refs):
    out_ref = refs[-1]
    at = 0
    for skip, ref in zip(skips, refs[:-1]):
        size = ref.shape[0] - skip
        out_ref[at : at + size] = ref[skip:]
        at += size


def pieces_kernel(count, order, *refs):
    pieces, rest = refs[:count], refs[count:]

    def grid(a):
        rows = []
        for at, lead in order:
            ref = pieces[at]
            where = lead + (a,) if len(ref.shape) == 6 else (a,)
            halves, tiles = ref.shape[-4:-2]
            for half in range(halves):
                rows.append(
                    jnp.concatenate(
                        [ref[where + (half, t)] for t in range(tiles)], axis=1
                    )
                )
        return jnp.concatenate(rows, axis=0)

    profile_body(grid, *rest)


def plain_kernel(pieces, *rest):
    profile_body(lambda a: pieces[a], *rest)


def shards(image_stack, steering, wiener_filter, range_group, lay_list, lay_count):
    halves, acq_share, azb_all, columns, pixels = image_stack.shape
    blocks = lay_list.shape[0]
    _, _, acquisitions, elevation = steering.shape
    depth = 2 * acquisitions
    chips = lax.axis_size("az")
    cores = lax.axis_size("acq")
    per_block = lay_list.shape[2]
    rows = blocks * per_block
    tiles = pixels // LANES
    pairwise = acq_share * columns == 16 and cores == 2 and chips & (chips - 1) == 0
    small = [range_group.reshape(1, columns), lay_count, lay_list, steering, wiener_filter]

    def prepare(small):
        return pl.pallas_call(
            lambda *refs: prepare_kernel(acq_share, pairwise, *refs),
            out_shape=[
                jax.ShapeDtypeStruct((columns, columns * depth, 2 * elevation), BF16),
                jax.ShapeDtypeStruct((columns, depth, 2 * elevation), BF16),
                jax.ShapeDtypeStruct((columns, 2 * elevation, depth), BF16),
                jax.ShapeDtypeStruct((columns, 2 * elevation, columns * depth), BF16),
                jax.ShapeDtypeStruct((columns, columns * depth, depth), BF16),
                jax.ShapeDtypeStruct((blocks * columns * per_block, pixels), BF16),
                jax.ShapeDtypeStruct((blocks * columns, 8, pixels), F32),
            ],
            in_specs=[VMEM] * len(small),
            out_specs=[VMEM] * 7,
            scratch_shapes=[pltpu.VMEM((depth, depth), F32)],
            cost_estimate=pl.CostEstimate(
                flops=1_000_000_000, bytes_accessed=4_000_000, transcendentals=0
            ),
            compiler_params=pltpu.CompilerParams(vmem_limit_bytes=16 << 20),
            name="prepare",
        )(*small)

    if pairwise:
        view = image_stack.reshape(halves, acq_share, azb_all, columns, tiles, LANES)
        view = view.transpose(0, 1, 2, 4, 3, 5)
        turns = sorted(range(1, chips), key=lambda d: (d < chips // 2, d))
        places = [[(0, 0)], [(0, 1)]] + [[(d, 0), (d, 1)] for d in turns]
        unit = (halves, tiles, acq_share, columns, LANES)
        outputs = [
            jax.ShapeDtypeStruct((len(owners) * blocks,) + unit, BF16) for owners in places
        ]
        relayed = pl.pallas_call(
            lambda *refs: relay_kernel(places, len(small), *refs),
            out_shape=outputs + [jax.ShapeDtypeStruct(x.shape, x.dtype) for x in small],
            in_specs=[HBM] * (1 + len(small)),
            out_specs=[VMEM] * (len(places) + len(small)),
            scratch_shapes=[
                pltpu.VMEM(view.shape, BF16),
                pltpu.SemaphoreType.DMA,
                pltpu.SemaphoreType.DMA((len(small),)),
            ],
            compiler_params=pltpu.CompilerParams(vmem_limit_bytes=4 << 20),
            name="relay",
        )(*[pltpu.with_memory_space_constraint(x, pltpu.HBM) for x in [view] + small])
        prepared = prepare(relayed[len(places) :])
        flat = (halves, tiles, acq_share * columns, LANES)
        chunks = [chunk.reshape((-1,) + flat) for chunk in relayed[: len(places)]]
        got, waiting = {(0, 0): chunks[0]}, {(0, 1): chunks[1]}
        for d, chunk in zip(turns, chunks[2:]):
            arrived = lax.ppermute(chunk, "az", [(c, c ^ d) for c in range(chips)])
            got[d, 0] = waiting[d, 1] = arrived
        names = list(waiting)
        skips = [waiting[n].shape[0] - blocks for n in names]
        passing = pl.pallas_call(
            lambda *refs: join_kernel(skips, *refs),
            out_shape=jax.ShapeDtypeStruct((len(names) * blocks,) + flat, BF16),
            in_specs=[VMEM] * len(names),
            out_specs=VMEM,
            compiler_params=pltpu.CompilerParams(vmem_limit_bytes=2 << 20),
            name="join",
        )(*[waiting[n] for n in names])
        passing, prepared = lax.optimization_barrier((passing, prepared))
        passed = lax.ppermute(passing, "acq", [(0, 1), (1, 0)])
        arrays, order = [], {}
        for place, array in got.items():
            order[place] = (len(arrays), ())
            arrays.append(array)
        for at, place in enumerate(names):
            order[place] = (len(arrays), (at,))
        arrays.append(passed.reshape((len(names), blocks) + flat))
        order = [order[d, j] for d in range(chips) for j in range(cores)]
        lead = arrays
        body = lambda *refs: pieces_kernel(len(arrays), order, *refs)
    else:
        moved = lax.all_to_all(
            image_stack, ("az", "acq"), split_axis=2, concat_axis=0, tiled=True
        )
        moved = moved.reshape(-1, acq_share, blocks, columns, pixels)
        lead = [moved.transpose(2, 0, 1, 3, 4).reshape(blocks, columns * depth, pixels)]
        body = plain_kernel
        prepared = prepare(small)

    return pl.pallas_call(
        body,
        out_shape=jax.ShapeDtypeStruct((blocks, columns, elevation, pixels), BF16),
        in_specs=[VMEM] * (len(lead) + len(prepared)),
        out_specs=ANY,
        scratch_shapes=[
            pltpu.VMEM((columns, rows, elevation), F32),
            pltpu.VMEM((columns, rows, elevation), F32),
            pltpu.VMEM((columns, rows, 2 * elevation), BF16),
            pltpu.VMEM((columns, rows, depth), F32),
            pltpu.VMEM((blocks, columns, elevation, pixels), BF16),
            pltpu.SemaphoreType.DMA,
        ],
        compiler_params=pltpu.CompilerParams(vmem_limit_bytes=24 << 20),
        cost_estimate=pl.CostEstimate(
            flops=2_000_000_000, bytes_accessed=4_000_000, transcendentals=0
        ),
        name="profiles",
    )(*lead, *prepared)


def solution(mesh):
    return jax.shard_map(
        shards,
        mesh=mesh,
        in_specs=(
            P(None, ("az", "acq"), "groups", "rg", None),
            P("rg", None, None, None),
            P("rg", None, None, None),
            P("rg"),
            P(("groups", "az", "acq"), "rg", None),
            P(("groups", "az", "acq"), "rg"),
        ),
        out_specs=P(("groups", "az", "acq"), "rg", None, None),
        check_vma=False,
    )
```

```python
import jax
import jax.numpy as jnp
from jax import lax
from jax.experimental import pallas as pl
from jax.experimental.pallas import tpu as pltpu
from jax.sharding import PartitionSpec as P

ITERS = 8
STEP_SIZE = 0.5
SHRINK = 0.25
LANES = 128
F32 = jnp.float32
BF16 = jnp.bfloat16

VMEM = pl.BlockSpec(memory_space=pltpu.VMEM)
ANY = pl.BlockSpec(memory_space=pl.ANY)
HBM = pl.BlockSpec(memory_space=pltpu.HBM)


def dot(a, b, contract=(1, 0)):
    return lax.dot_general(
        a, b, (((contract[0],), (contract[1],)), ((), ())), preferred_element_type=F32
    )


def relay_kernel(places, extra, x_ref, *refs):
    inputs, refs = refs[:extra], refs[extra:]
    chunks, fetched = refs[: len(places)], refs[len(places) : len(places) + extra]
    stack_ref, stack_sem, sems = refs[len(places) + extra :]
    halves, acq_share, _, tiles = x_ref.shape[:4]
    whole = pltpu.make_async_copy(x_ref, stack_ref, stack_sem)
    whole.start()
    copies = [
        pltpu.make_async_copy(source, target, sems.at[at])
        for at, (source, target) in enumerate(zip(inputs, fetched))
    ]
    for copy in copies:
        copy.start()
    chip, core = lax.axis_index("az"), lax.axis_index("acq")
    cores = lax.axis_size("acq")
    whole.wait()
    for owners, chunk in zip(places, chunks):
        blocks = chunk.shape[0] // len(owners)
        for at, (d, j) in enumerate(owners):
            first = ((chip ^ d) * cores + (core ^ j)) * blocks
            for a in range(blocks):
                for half in range(halves):
                    for t in range(tiles):
                        for acq in range(acq_share):
                            chunk[at * blocks + a, half, t, acq] = stack_ref[
                                half, acq, first + a, t
                            ]
    for copy in copies:
        copy.wait()


def prepare_kernel(
    acq_share, relative, groups, counts, list_ref, steer_ref, filter_ref,
    first_ref, half_op_ref, op_t_ref, wiener_ref, select_ref, chosen_ref, clear_ref, fmat_ref,
):
    group_count, _, acquisitions, elevation = steer_ref.shape
    blocks, columns, per_block = list_ref.shape
    depth = 2 * acquisitions
    pixels = chosen_ref.shape[0] * LANES
    first_group = lax.axis_index("rg") * group_count
    row = lax.broadcasted_iota(jnp.int32, (per_block, per_block), 0)
    lane = lax.broadcasted_iota(jnp.int32, (per_block, per_block), 1)
    entry = lax.broadcasted_iota(jnp.int32, (per_block, pixels), 0)
    pixel = lax.broadcasted_iota(jnp.int32, (per_block, pixels), 1)
    for a in range(blocks):
        for r in range(columns):
            listed = list_ref[a, r : r + 1].astype(F32)
            upright = jnp.sum(jnp.where(row == lane, listed, 0.0), axis=1, keepdims=True)
            usable = entry < counts[a : a + 1, r : r + 1]
            hit = (upright.astype(jnp.int32) == pixel) & usable
            chosen = jnp.where(hit, 1.0, 0.0).astype(F32)
            start = (a * columns + r) * per_block
            for t in range(pixels // LANES):
                part = chosen[:, t * LANES : (t + 1) * LANES]
                chosen_ref[t, start : start + per_block] = part.astype(BF16)
            covered = jnp.sum(chosen, axis=0, keepdims=True)
            clear_ref[a * columns + r] = jnp.broadcast_to(1.0 - covered, clear_ref.shape[1:])
    at = lax.broadcasted_iota(jnp.int32, (1, depth), 1)
    half, acq = at // acquisitions, at % acquisitions
    source = acq // acq_share
    if relative:
        cores = lax.axis_size("acq")
        chip, core = lax.axis_index("az"), lax.axis_index("acq")
        source = ((source // cores) ^ chip) * cores + ((source % cores) ^ core)
    place = ((source * 2 + half) * acq_share + acq % acq_share) * columns
    long = lax.broadcasted_iota(jnp.int32, (columns * depth, depth), 0)
    for r in range(columns):
        g = jnp.max(groups[:, r : r + 1]) - first_group
        select = jnp.where(long == place + r, 1.0, 0.0).astype(BF16)
        select_ref[r] = select
        real = steer_ref[g, 0]
        imag = steer_ref[g, 1]
        slabs = []
        for at in range(0, elevation, LANES):
            re, im = real[:, at : at + LANES], imag[:, at : at + LANES]
            slabs += [jnp.concatenate([re, im], axis=0), jnp.concatenate([-im, re], axis=0)]
        operator = jnp.concatenate(slabs, axis=1)
        half_op = operator * jnp.asarray(STEP_SIZE, BF16)
        first = dot(select, half_op).astype(BF16)
        op_t = jnp.transpose(operator.astype(F32)).astype(BF16)
        for slab in range(op_t_ref.shape[1]):
            op_t_ref[r, slab] = op_t[slab * 2 * LANES : (slab + 1) * 2 * LANES]
        for slab in range(len(slabs)):
            half_op_ref[r, slab] = half_op[:, slab * LANES : (slab + 1) * LANES]
            first_ref[r, slab] = first[:, slab * LANES : (slab + 1) * LANES]
        fmat_ref[:acquisitions, :acquisitions] = filter_ref[g, 0].astype(F32)
        fmat_ref[:acquisitions, acquisitions:] = -filter_ref[g, 1].astype(F32)
        fmat_ref[acquisitions:, :acquisitions] = filter_ref[g, 1].astype(F32)
        fmat_ref[acquisitions:, acquisitions:] = filter_ref[g, 0].astype(F32)
        spread = dot(fmat_ref[...].astype(BF16), select, (1, 1)).astype(BF16)
        wiener = dot(op_t, spread).astype(BF16)
        for slab in range(wiener_ref.shape[1]):
            wiener_ref[r, slab] = wiener[:, slab * LANES : (slab + 1) * LANES]


def wide(ref, *at):
    return jnp.concatenate([ref[where] for where in at], axis=-1)


def profile_body(
    grid, first_ref, half_op_ref, op_t_ref, wiener_ref, select_ref, chosen_ref, clear_ref,
    out_ref, real_ref, imag_ref, rounded_ref, target_ref, image_ref, sem,
):
    blocks, columns, elevation, _ = out_ref.shape
    tiles, entries = chosen_ref.shape[:2]
    per_block = entries // (blocks * columns)
    slabs = elevation // LANES

    def chosen(first, size):
        return wide(chosen_ref, *[(t, slice(first, first + size)) for t in range(tiles)])

    share = columns * per_block
    picked = [
        dot(chosen(a * share, share), grid(a), (1, 1)).astype(BF16) for a in range(blocks)
    ]
    picked = [
        jnp.concatenate([p[r * per_block : (r + 1) * per_block] for p in picked], axis=0)
        for r in range(columns)
    ]
    for r in range(columns):
        target_ref[r] = dot(picked[r], select_ref[r])

    def predicted(r):
        size = rounded_ref.shape[2]
        deep = op_t_ref.shape[2] // LANES
        total = None
        for at in range(0, op_t_ref.shape[1], 2):
            stacked = jnp.concatenate(
                [
                    wide(rounded_ref, *[(r, (at + j) * deep + k) for k in range(deep)])
                    for j in range(2)
                ],
                axis=0,
            )
            both = dot(stacked, wide(op_t_ref, (r, at), (r, at + 1)))
            total = both if total is None else total + both
        depth = op_t_ref.shape[3]
        return total[:size, :depth] + total[size:, depth:]

    def update(r, misfit, op_ref, first):
        for slab in range(slabs):
            z = dot(misfit, wide(op_ref, (r, 2 * slab), (r, 2 * slab + 1)))
            zr, zi = z[:, :LANES], z[:, LANES:]
            if not first:
                zr = zr + real_ref[r, slab]
                zi = zi + imag_ref[r, slab]
            magnitude = zr * zr + zi * zi
            factor = jnp.maximum(
                1.0 - SHRINK * lax.rsqrt(jnp.maximum(magnitude, SHRINK * SHRINK)), 0.0
            )
            xr = zr * factor
            xi = zi * factor
            real_ref[r, slab] = xr
            imag_ref[r, slab] = xi
            rounded_ref[r, 2 * slab] = xr.astype(BF16)
            rounded_ref[r, 2 * slab + 1] = xi.astype(BF16)

    shares = [
        (a, r, slab) for a in range(blocks) for slab in range(slabs) for r in range(columns)
    ]

    def wiener(a, r, slab):
        first = 2 * slab * LANES
        depths = range(wiener_ref.shape[1])
        br = dot(wide(wiener_ref, *[(r, k, slice(first, first + LANES)) for k in depths]), grid(a))
        first += LANES
        bi = dot(wide(wiener_ref, *[(r, k, slice(first, first + LANES)) for k in depths]), grid(a))
        power = (br * br + bi * bi) * clear_ref[a * columns + r, :1]
        power = power.astype(BF16)
        image_ref[a, r, slab * LANES : (slab + 1) * LANES] = power

    todo = list(shares)

    def more(count):
        for part in todo[:count]:
            wiener(*part)
        del todo[:count]

    each = len(shares) // ITERS
    for t in range(ITERS):
        if t == 0:
            misfits = picked
        else:
            misfits = [(target_ref[r] - predicted(r)).astype(BF16) for r in range(columns)]
        for r in range(columns):
            update(r, misfits[r], half_op_ref if t else first_ref, t == 0)
            more(each // columns)

    def copies(a, r, slab):
        where = pl.ds(slab * LANES, LANES)
        return [
            pltpu.make_async_copy(image_ref.at[a, r, where], out_ref.at[a, r, where], sem)
        ]

    for r in range(columns):
        for a in range(blocks):
            rows = slice(a * per_block, (a + 1) * per_block)
            for slab in range(slabs):
                xr, xi = real_ref[r, slab, rows], imag_ref[r, slab, rows]
                strength = (xr * xr + xi * xi).astype(BF16)
                placed = dot(
                    strength, chosen((a * columns + r) * per_block, per_block), (0, 0)
                ).astype(BF16)
                where = slice(slab * LANES, (slab + 1) * LANES)
                image_ref[a, r, where] = image_ref[a, r, where] + placed
                for copy in copies(a, r, slab):
                    copy.start()
    for a in range(blocks):
        for r in range(columns):
            for slab in range(slabs):
                for copy in copies(a, r, slab):
                    copy.wait()


def join_kernel(skips, *refs):
    out_ref = refs[-1]
    at = 0
    for skip, ref in zip(skips, refs[:-1]):
        size = ref.shape[0] - skip
        out_ref[at : at + size] = ref[skip:]
        at += size


def pieces_kernel(count, order, *refs):
    pieces, rest = refs[:count], refs[count:]

    def grid(a):
        rows = []
        for at, lead in order:
            ref = pieces[at]
            where = lead + (a,) if len(ref.shape) == 6 else (a,)
            halves, tiles = ref.shape[-4:-2]
            for half in range(halves):
                rows.append(
                    jnp.concatenate(
                        [ref[where + (half, t)] for t in range(tiles)], axis=1
                    )
                )
        return jnp.concatenate(rows, axis=0)

    profile_body(grid, *rest)


def plain_kernel(pieces, *rest):
    profile_body(lambda a: pieces[a], *rest)


def shards(image_stack, steering, wiener_filter, range_group, lay_list, lay_count):
    halves, acq_share, azb_all, columns, pixels = image_stack.shape
    blocks = lay_list.shape[0]
    _, _, acquisitions, elevation = steering.shape
    depth = 2 * acquisitions
    chips = lax.axis_size("az")
    cores = lax.axis_size("acq")
    per_block = lay_list.shape[2]
    rows = blocks * per_block
    tiles = pixels // LANES
    slabs = 2 * elevation // LANES
    pairwise = acq_share * columns == 16 and cores == 2 and chips & (chips - 1) == 0
    small = [range_group.reshape(1, columns), lay_count, lay_list, steering, wiener_filter]

    def prepare(small):
        return pl.pallas_call(
            lambda *refs: prepare_kernel(acq_share, pairwise, *refs),
            out_shape=[
                jax.ShapeDtypeStruct((columns, slabs, columns * depth, LANES), BF16),
                jax.ShapeDtypeStruct((columns, slabs, depth, LANES), BF16),
                jax.ShapeDtypeStruct((columns, slabs // 2, 2 * LANES, depth), BF16),
                jax.ShapeDtypeStruct(
                    (columns, columns * depth // LANES, 2 * elevation, LANES), BF16
                ),
                jax.ShapeDtypeStruct((columns, columns * depth, depth), BF16),
                jax.ShapeDtypeStruct((tiles, blocks * columns * per_block, LANES), BF16),
                jax.ShapeDtypeStruct((blocks * columns, 8, pixels), F32),
            ],
            in_specs=[VMEM] * len(small),
            out_specs=[VMEM] * 7,
            scratch_shapes=[pltpu.VMEM((depth, depth), F32)],
            cost_estimate=pl.CostEstimate(
                flops=1_000_000_000, bytes_accessed=4_000_000, transcendentals=0
            ),
            compiler_params=pltpu.CompilerParams(vmem_limit_bytes=16 << 20),
            name="prepare",
        )(*small)

    if pairwise:
        view = image_stack.reshape(halves, acq_share, azb_all, columns, tiles, LANES)
        view = view.transpose(0, 1, 2, 4, 3, 5)
        turns = sorted(range(1, chips), key=lambda d: (d < chips // 2, d))
        places = [[(0, 0)], [(0, 1)]] + [[(d, 0), (d, 1)] for d in turns]
        unit = (halves, tiles, acq_share, columns, LANES)
        outputs = [
            jax.ShapeDtypeStruct((len(owners) * blocks,) + unit, BF16) for owners in places
        ]
        relayed = pl.pallas_call(
            lambda *refs: relay_kernel(places, len(small), *refs),
            out_shape=outputs + [jax.ShapeDtypeStruct(x.shape, x.dtype) for x in small],
            in_specs=[HBM] * (1 + len(small)),
            out_specs=[VMEM] * (len(places) + len(small)),
            scratch_shapes=[
                pltpu.VMEM(view.shape, BF16),
                pltpu.SemaphoreType.DMA,
                pltpu.SemaphoreType.DMA((len(small),)),
            ],
            compiler_params=pltpu.CompilerParams(vmem_limit_bytes=4 << 20),
            name="relay",
        )(*[pltpu.with_memory_space_constraint(x, pltpu.HBM) for x in [view] + small])
        prepared = prepare(relayed[len(places) :])
        flat = (halves, tiles, acq_share * columns, LANES)
        chunks = [chunk.reshape((-1,) + flat) for chunk in relayed[: len(places)]]
        got, waiting = {(0, 0): chunks[0]}, {(0, 1): chunks[1]}
        for d, chunk in zip(turns, chunks[2:]):
            arrived = lax.ppermute(chunk, "az", [(c, c ^ d) for c in range(chips)])
            got[d, 0] = waiting[d, 1] = arrived
        names = list(waiting)
        skips = [waiting[n].shape[0] - blocks for n in names]
        passing = pl.pallas_call(
            lambda *refs: join_kernel(skips, *refs),
            out_shape=jax.ShapeDtypeStruct((len(names) * blocks,) + flat, BF16),
            in_specs=[VMEM] * len(names),
            out_specs=VMEM,
            compiler_params=pltpu.CompilerParams(vmem_limit_bytes=2 << 20),
            name="join",
        )(*[waiting[n] for n in names])
        passing, prepared = lax.optimization_barrier((passing, prepared))
        passed = lax.ppermute(passing, "acq", [(0, 1), (1, 0)])
        arrays, order = [], {}
        for place, array in got.items():
            order[place] = (len(arrays), ())
            arrays.append(array)
        for at, place in enumerate(names):
            order[place] = (len(arrays), (at,))
        arrays.append(passed.reshape((len(names), blocks) + flat))
        order = [order[d, j] for d in range(chips) for j in range(cores)]
        lead = arrays
        body = lambda *refs: pieces_kernel(len(arrays), order, *refs)
    else:
        moved = lax.all_to_all(
            image_stack, ("az", "acq"), split_axis=2, concat_axis=0, tiled=True
        )
        moved = moved.reshape(-1, acq_share, blocks, columns, pixels)
        lead = [moved.transpose(2, 0, 1, 3, 4).reshape(blocks, columns * depth, pixels)]
        body = plain_kernel
        prepared = prepare(small)

    return pl.pallas_call(
        body,
        out_shape=jax.ShapeDtypeStruct((blocks, columns, elevation, pixels), BF16),
        in_specs=[VMEM] * (len(lead) + len(prepared)),
        out_specs=ANY,
        scratch_shapes=[
            pltpu.VMEM((columns, slabs // 2, rows, LANES), F32),
            pltpu.VMEM((columns, slabs // 2, rows, LANES), F32),
            pltpu.VMEM((columns, slabs, rows, LANES), BF16),
            pltpu.VMEM((columns, rows, depth), F32),
            pltpu.VMEM((blocks, columns, elevation, pixels), BF16),
            pltpu.SemaphoreType.DMA,
        ],
        compiler_params=pltpu.CompilerParams(vmem_limit_bytes=24 << 20),
        cost_estimate=pl.CostEstimate(
            flops=2_000_000_000, bytes_accessed=4_000_000, transcendentals=0
        ),
        name="profiles",
    )(*lead, *prepared)


def solution(mesh):
    return jax.shard_map(
        shards,
        mesh=mesh,
        in_specs=(
            P(None, ("az", "acq"), "groups", "rg", None),
            P("rg", None, None, None),
            P("rg", None, None, None),
            P("rg"),
            P(("groups", "az", "acq"), "rg", None),
            P(("groups", "az", "acq"), "rg"),
        ),
        out_specs=P(("groups", "az", "acq"), "rg", None, None),
        check_vma=False,
    )
```

```python
import jax
import jax.numpy as jnp
from jax import lax
from jax.experimental import pallas as pl
from jax.experimental.pallas import tpu as pltpu
from jax.sharding import PartitionSpec as P

ITERS = 8
STEP_SIZE = 0.5
SHRINK = 0.25
LANES = 128
F32 = jnp.float32
BF16 = jnp.bfloat16

VMEM = pl.BlockSpec(memory_space=pltpu.VMEM)
ANY = pl.BlockSpec(memory_space=pl.ANY)
HBM = pl.BlockSpec(memory_space=pltpu.HBM)


def dot(a, b, contract=(1, 0)):
    return lax.dot_general(
        a, b, (((contract[0],), (contract[1],)), ((), ())), preferred_element_type=F32
    )


def turns_of(chips):
    if chips == 4:
        return [[1, 3, 0, 2], [3, 2, 1, 0], [2, 0, 3, 1]]
    far = sorted(range(1, chips), key=lambda d: (d < chips // 2, d))
    return [[c ^ d for c in range(chips)] for d in far]


def pick(table, index):
    return sum(jnp.where(index == at, value, 0) for at, value in enumerate(table))


def relay_kernel(places, x_ref, *refs):
    chunks, stack_ref, sem = refs[:-2], refs[-2], refs[-1]
    whole = pltpu.make_async_copy(x_ref, stack_ref, sem)
    whole.start()
    chip, core = lax.axis_index("az"), lax.axis_index("acq")
    cores = lax.axis_size("acq")
    whole.wait()
    cut(places, chip, core, cores, stack_ref, chunks)


def cut(places, chip, core, cores, stack_ref, chunks):
    halves, acq_share, _, tiles = stack_ref.shape[:4]
    for owners, chunk in zip(places, chunks):
        blocks = chunk.shape[0] // len(owners)
        for at, (turn, j) in enumerate(owners):
            owner = chip if turn is None else pick(turns_of(lax.axis_size("az"))[turn], chip)
            first = (owner * cores + (core ^ j)) * blocks
            for a in range(blocks):
                for half in range(halves):
                    for t in range(tiles):
                        for acq in range(acq_share):
                            chunk[at * blocks + a, half, t, acq] = stack_ref[
                                half, acq, first + a, t
                            ]


def prepare_kernel(
    acq_share, relative, groups_in, counts_in, list_in, steer_in, filter_in,
    first_ref, half_op_ref, op_t_ref, wiener_ref, select_ref, chosen_ref, clear_ref,
    fmat_ref, groups, counts, list_ref, steer_ref, filter_ref, sems,
):
    fetched = [
        pltpu.make_async_copy(source, target, sems.at[at])
        for at, (source, target) in enumerate(
            [
                (groups_in, groups), (counts_in, counts), (list_in, list_ref),
                (steer_in, steer_ref), (filter_in, filter_ref),
            ]
        )
    ]
    for copy in fetched:
        copy.start()
    for copy in fetched:
        copy.wait()

    group_count, _, acquisitions, elevation = steer_ref.shape
    blocks, columns, per_block = list_ref.shape
    depth = 2 * acquisitions
    pixels = chosen_ref.shape[0] * LANES
    first_group = lax.axis_index("rg") * group_count
    row = lax.broadcasted_iota(jnp.int32, (per_block, per_block), 0)
    lane = lax.broadcasted_iota(jnp.int32, (per_block, per_block), 1)
    entry = lax.broadcasted_iota(jnp.int32, (per_block, pixels), 0)
    pixel = lax.broadcasted_iota(jnp.int32, (per_block, pixels), 1)
    for a in range(blocks):
        for r in range(columns):
            listed = list_ref[a, r : r + 1].astype(F32)
            upright = jnp.sum(jnp.where(row == lane, listed, 0.0), axis=1, keepdims=True)
            usable = entry < counts[a : a + 1, r : r + 1]
            hit = (upright.astype(jnp.int32) == pixel) & usable
            chosen = jnp.where(hit, 1.0, 0.0).astype(F32)
            start = (a * columns + r) * per_block
            for t in range(pixels // LANES):
                part = chosen[:, t * LANES : (t + 1) * LANES]
                chosen_ref[t, start : start + per_block] = part.astype(BF16)
            covered = jnp.sum(chosen, axis=0, keepdims=True)
            clear_ref[a * columns + r] = jnp.broadcast_to(1.0 - covered, clear_ref.shape[1:])
    at = lax.broadcasted_iota(jnp.int32, (1, depth), 1)
    half, acq = at // acquisitions, at % acquisitions
    source = acq // acq_share
    if relative:
        cores, chips = lax.axis_size("acq"), lax.axis_size("az")
        chip, core = lax.axis_index("az"), lax.axis_index("acq")
        arrival = jnp.zeros_like(source)
        for turn, targets in enumerate(turns_of(chips)):
            sender = pick([targets.index(c) for c in range(chips)], chip)
            arrival = jnp.where(source // cores == sender, turn + 1, arrival)
        source = arrival * cores + ((source % cores) ^ core)
    place = ((source * 2 + half) * acq_share + acq % acq_share) * columns
    long = lax.broadcasted_iota(jnp.int32, (columns * depth, depth), 0)
    for r in range(columns):
        g = jnp.clip(jnp.max(groups[:, r : r + 1]) - first_group, 0, group_count - 1)
        select = jnp.where(long == place + r, 1.0, 0.0).astype(BF16)
        select_ref[r] = select
        real = steer_ref[g, 0]
        imag = steer_ref[g, 1]
        slabs = []
        for at in range(0, elevation, LANES):
            re, im = real[:, at : at + LANES], imag[:, at : at + LANES]
            slabs += [jnp.concatenate([re, im], axis=0), jnp.concatenate([-im, re], axis=0)]
        operator = jnp.concatenate(slabs, axis=1)
        half_op = operator * jnp.asarray(STEP_SIZE, BF16)
        first = dot(select, half_op).astype(BF16)
        op_t = jnp.transpose(operator.astype(F32)).astype(BF16)
        for slab in range(op_t_ref.shape[1]):
            op_t_ref[r, slab] = op_t[slab * 2 * LANES : (slab + 1) * 2 * LANES]
        for slab in range(len(slabs)):
            half_op_ref[r, slab] = half_op[:, slab * LANES : (slab + 1) * LANES]
            first_ref[r, slab] = first[:, slab * LANES : (slab + 1) * LANES]
        fmat_ref[:acquisitions, :acquisitions] = filter_ref[g, 0].astype(F32)
        fmat_ref[:acquisitions, acquisitions:] = -filter_ref[g, 1].astype(F32)
        fmat_ref[acquisitions:, :acquisitions] = filter_ref[g, 1].astype(F32)
        fmat_ref[acquisitions:, acquisitions:] = filter_ref[g, 0].astype(F32)
        spread = dot(fmat_ref[...].astype(BF16), select, (1, 1)).astype(BF16)
        wiener = dot(op_t, spread).astype(BF16)
        for slab in range(wiener_ref.shape[1]):
            wiener_ref[r, slab] = wiener[:, slab * LANES : (slab + 1) * LANES]


def wide(ref, *at):
    return jnp.concatenate([ref[where] for where in at], axis=-1)


def profile_body(
    grid, first_ref, half_op_ref, op_t_ref, wiener_ref, select_ref, chosen_ref, clear_ref,
    out_ref, real_ref, imag_ref, rounded_ref, target_ref, image_ref, sem,
):
    blocks, columns, elevation, _ = out_ref.shape
    tiles, entries = chosen_ref.shape[:2]
    per_block = entries // (blocks * columns)
    slabs = elevation // LANES

    def chosen(first, size):
        return wide(chosen_ref, *[(t, slice(first, first + size)) for t in range(tiles)])

    share = columns * per_block
    picked = [
        dot(chosen(a * share, share), grid(a), (1, 1)).astype(BF16) for a in range(blocks)
    ]
    picked = [
        jnp.concatenate([p[r * per_block : (r + 1) * per_block] for p in picked], axis=0)
        for r in range(columns)
    ]
    for r in range(columns):
        target_ref[r] = dot(picked[r], select_ref[r])

    def predicted(r):
        size = rounded_ref.shape[2]
        deep = op_t_ref.shape[2] // LANES
        total = None
        for at in range(0, op_t_ref.shape[1], 2):
            stacked = jnp.concatenate(
                [
                    wide(rounded_ref, *[(r, (at + j) * deep + k) for k in range(deep)])
                    for j in range(2)
                ],
                axis=0,
            )
            both = dot(stacked, wide(op_t_ref, (r, at), (r, at + 1)))
            total = both if total is None else total + both
        depth = op_t_ref.shape[3]
        return total[:size, :depth] + total[size:, depth:]

    def update(r, misfit, op_ref, first):
        for slab in range(slabs):
            z = dot(misfit, wide(op_ref, (r, 2 * slab), (r, 2 * slab + 1)))
            zr, zi = z[:, :LANES], z[:, LANES:]
            if not first:
                zr = zr + real_ref[r, slab]
                zi = zi + imag_ref[r, slab]
            magnitude = zr * zr + zi * zi
            factor = jnp.maximum(
                1.0 - SHRINK * lax.rsqrt(jnp.maximum(magnitude, SHRINK * SHRINK)), 0.0
            )
            xr = zr * factor
            xi = zi * factor
            real_ref[r, slab] = xr
            imag_ref[r, slab] = xi
            rounded_ref[r, 2 * slab] = xr.astype(BF16)
            rounded_ref[r, 2 * slab + 1] = xi.astype(BF16)

    shares = [
        (a, r, slab) for a in range(blocks) for slab in range(slabs) for r in range(columns)
    ]

    def wiener(a, r, slab):
        first = 2 * slab * LANES
        depths = range(wiener_ref.shape[1])
        br = dot(wide(wiener_ref, *[(r, k, slice(first, first + LANES)) for k in depths]), grid(a))
        first += LANES
        bi = dot(wide(wiener_ref, *[(r, k, slice(first, first + LANES)) for k in depths]), grid(a))
        power = (br * br + bi * bi) * clear_ref[a * columns + r, :1]
        power = power.astype(BF16)
        image_ref[a, r, slab * LANES : (slab + 1) * LANES] = power

    todo = list(shares)

    def more(count):
        for part in todo[:count]:
            wiener(*part)
        del todo[:count]

    for t in range(ITERS):
        if t == 0:
            misfits = picked
        else:
            misfits = [(target_ref[r] - predicted(r)).astype(BF16) for r in range(columns)]
        for r in range(columns):
            more(1)
            update(r, misfits[r], half_op_ref if t else first_ref, t == 0)

    def copies(a, r, slab):
        where = pl.ds(slab * LANES, LANES)
        return [
            pltpu.make_async_copy(image_ref.at[a, r, where], out_ref.at[a, r, where], sem)
        ]

    for r in range(columns):
        for a in range(blocks):
            rows = slice(a * per_block, (a + 1) * per_block)
            for slab in range(slabs):
                xr, xi = real_ref[r, slab, rows], imag_ref[r, slab, rows]
                strength = (xr * xr + xi * xi).astype(BF16)
                placed = dot(
                    strength, chosen((a * columns + r) * per_block, per_block), (0, 0)
                ).astype(BF16)
                where = slice(slab * LANES, (slab + 1) * LANES)
                image_ref[a, r, where] = image_ref[a, r, where] + placed
                for copy in copies(a, r, slab):
                    copy.start()
    for a in range(blocks):
        for r in range(columns):
            for slab in range(slabs):
                for copy in copies(a, r, slab):
                    copy.wait()


def join_kernel(skips, *refs):
    out_ref = refs[-1]
    at = 0
    for skip, ref in zip(skips, refs[:-1]):
        size = ref.shape[0] - skip
        out_ref[at : at + size] = ref[skip:]
        at += size


def pieces_kernel(count, order, *refs):
    pieces, rest = refs[:count], refs[count:]

    def grid(a):
        rows = []
        for at, lead in order:
            ref = pieces[at]
            where = lead + (a,) if len(ref.shape) == 6 else (a,)
            halves, tiles = ref.shape[-4:-2]
            for half in range(halves):
                rows.append(
                    jnp.concatenate(
                        [ref[where + (half, t)] for t in range(tiles)], axis=1
                    )
                )
        return jnp.concatenate(rows, axis=0)

    profile_body(grid, *rest)


def plain_kernel(pieces, *rest):
    profile_body(lambda a: pieces[a], *rest)


def shards(image_stack, steering, wiener_filter, range_group, lay_list, lay_count):
    halves, acq_share, azb_all, columns, pixels = image_stack.shape
    blocks = lay_list.shape[0]
    _, _, acquisitions, elevation = steering.shape
    depth = 2 * acquisitions
    chips = lax.axis_size("az")
    cores = lax.axis_size("acq")
    per_block = lay_list.shape[2]
    rows = blocks * per_block
    tiles = pixels // LANES
    slabs = 2 * elevation // LANES
    pairwise = acq_share * columns == 16 and cores == 2 and chips & (chips - 1) == 0
    small = [range_group.reshape(1, columns), lay_count, lay_list, steering, wiener_filter]

    def prepare(small):
        return pl.pallas_call(
            lambda *refs: prepare_kernel(acq_share, pairwise, *refs),
            out_shape=[
                jax.ShapeDtypeStruct((columns, slabs, columns * depth, LANES), BF16),
                jax.ShapeDtypeStruct((columns, slabs, depth, LANES), BF16),
                jax.ShapeDtypeStruct((columns, slabs // 2, 2 * LANES, depth), BF16),
                jax.ShapeDtypeStruct(
                    (columns, columns * depth // LANES, 2 * elevation, LANES), BF16
                ),
                jax.ShapeDtypeStruct((columns, columns * depth, depth), BF16),
                jax.ShapeDtypeStruct((tiles, blocks * columns * per_block, LANES), BF16),
                jax.ShapeDtypeStruct((blocks * columns, 8, pixels), F32),
            ],
            in_specs=[HBM] * len(small),
            out_specs=[VMEM] * 7,
            scratch_shapes=[pltpu.VMEM((depth, depth), F32)]
            + [pltpu.VMEM(x.shape, x.dtype) for x in small]
            + [pltpu.SemaphoreType.DMA((len(small),))],
            cost_estimate=pl.CostEstimate(
                flops=1_000_000_000, bytes_accessed=4_000_000, transcendentals=0
            ),
            compiler_params=pltpu.CompilerParams(vmem_limit_bytes=16 << 20),
            name="prepare",
        )(*[pltpu.with_memory_space_constraint(x, pltpu.HBM) for x in small])

    if pairwise:
        view = image_stack.reshape(halves, acq_share, azb_all, columns, tiles, LANES)
        view = view.transpose(0, 1, 2, 4, 3, 5)
        turns = turns_of(chips)
        places = [[(None, 0)], [(None, 1)]]
        places += [[(turn, 0), (turn, 1)] for turn in range(len(turns))]
        unit = (halves, tiles, acq_share, columns, LANES)
        outputs = [
            jax.ShapeDtypeStruct((len(owners) * blocks,) + unit, BF16) for owners in places
        ]
        relayed = pl.pallas_call(
            lambda *refs: relay_kernel(places, *refs),
            out_shape=outputs,
            in_specs=[HBM],
            out_specs=[VMEM] * len(places),
            scratch_shapes=[pltpu.VMEM(view.shape, BF16), pltpu.SemaphoreType.DMA],
            compiler_params=pltpu.CompilerParams(vmem_limit_bytes=4 << 20),
            name="relay",
        )(pltpu.with_memory_space_constraint(view, pltpu.HBM))
        prepared = prepare(small)
        flat = (halves, tiles, acq_share * columns, LANES)
        chunks = [chunk.reshape((-1,) + flat) for chunk in relayed]
        got, waiting = {(0, 0): chunks[0]}, {(0, 1): chunks[1]}
        for at, (targets, chunk) in enumerate(zip(turns, chunks[2:])):
            arrived = lax.ppermute(chunk, "az", list(enumerate(targets)))
            got[at + 1, 0] = waiting[at + 1, 1] = arrived
        names = list(waiting)
        skips = [waiting[n].shape[0] - blocks for n in names]
        passing = pl.pallas_call(
            lambda *refs: join_kernel(skips, *refs),
            out_shape=jax.ShapeDtypeStruct((len(names) * blocks,) + flat, BF16),
            in_specs=[VMEM] * len(names),
            out_specs=VMEM,
            compiler_params=pltpu.CompilerParams(vmem_limit_bytes=2 << 20),
            name="join",
        )(*[waiting[n] for n in names])
        passing, prepared = lax.optimization_barrier((passing, prepared))
        passed = lax.ppermute(passing, "acq", [(0, 1), (1, 0)])
        arrays, order = [], {}
        for place, array in got.items():
            order[place] = (len(arrays), ())
            arrays.append(array)
        for at, place in enumerate(names):
            order[place] = (len(arrays), (at,))
        arrays.append(passed.reshape((len(names), blocks) + flat))
        order = [order[d, j] for d in range(chips) for j in range(cores)]
        lead = arrays
        body = lambda *refs: pieces_kernel(len(arrays), order, *refs)
    else:
        moved = lax.all_to_all(
            image_stack, ("az", "acq"), split_axis=2, concat_axis=0, tiled=True
        )
        moved = moved.reshape(-1, acq_share, blocks, columns, pixels)
        lead = [moved.transpose(2, 0, 1, 3, 4).reshape(blocks, columns * depth, pixels)]
        body = plain_kernel
        prepared = prepare(small)

    return pl.pallas_call(
        body,
        out_shape=jax.ShapeDtypeStruct((blocks, columns, elevation, pixels), BF16),
        in_specs=[VMEM] * (len(lead) + len(prepared)),
        out_specs=ANY,
        scratch_shapes=[
            pltpu.VMEM((columns, slabs // 2, rows, LANES), F32),
            pltpu.VMEM((columns, slabs // 2, rows, LANES), F32),
            pltpu.VMEM((columns, slabs, rows, LANES), BF16),
            pltpu.VMEM((columns, rows, depth), F32),
            pltpu.VMEM((blocks, columns, elevation, pixels), BF16),
            pltpu.SemaphoreType.DMA,
        ],
        compiler_params=pltpu.CompilerParams(vmem_limit_bytes=24 << 20),
        cost_estimate=pl.CostEstimate(
            flops=2_000_000_000, bytes_accessed=4_000_000, transcendentals=0
        ),
        name="profiles",
    )(*lead, *prepared)


def solution(mesh):
    return jax.shard_map(
        shards,
        mesh=mesh,
        in_specs=(
            P(None, ("az", "acq"), "groups", "rg", None),
            P("rg", None, None, None),
            P("rg", None, None, None),
            P("rg"),
            P(("groups", "az", "acq"), "rg", None),
            P(("groups", "az", "acq"), "rg"),
        ),
        out_specs=P(("groups", "az", "acq"), "rg", None, None),
        check_vma=False,
    )
```

```python
import jax
import jax.numpy as jnp
from jax import lax
from jax.experimental import pallas as pl
from jax.experimental.pallas import tpu as pltpu
from jax.sharding import PartitionSpec as P

ITERS = 8
STEP_SIZE = 0.5
SHRINK = 0.25
LANES = 128
F32 = jnp.float32
BF16 = jnp.bfloat16

VMEM = pl.BlockSpec(memory_space=pltpu.VMEM)
ANY = pl.BlockSpec(memory_space=pl.ANY)
HBM = pl.BlockSpec(memory_space=pltpu.HBM)


def dot(a, b, contract=(1, 0)):
    return lax.dot_general(
        a, b, (((contract[0],), (contract[1],)), ((), ())), preferred_element_type=F32
    )


def turns_of(chips):
    if chips == 4:
        return [[1, 3, 0, 2], [3, 2, 1, 0], [2, 0, 3, 1]]
    far = sorted(range(1, chips), key=lambda d: (d < chips // 2, d))
    return [[c ^ d for c in range(chips)] for d in far]


def pick(table, index):
    return sum(jnp.where(index == at, value, 0) for at, value in enumerate(table))


def relay_kernel(places, extra, x_ref, *refs):
    small, refs = refs[:extra], refs[extra:]
    chunks, fetched, (stack_ref, sem, sems) = refs[: len(places)], refs[len(places) : -3], refs[-3:]
    whole = pltpu.make_async_copy(x_ref, stack_ref, sem)
    whole.start()
    copies = [
        pltpu.make_async_copy(source, target, sems.at[at])
        for at, (source, target) in enumerate(zip(small, fetched))
    ]
    for copy in copies:
        copy.start()
    chip, core = lax.axis_index("az"), lax.axis_index("acq")
    cores = lax.axis_size("acq")
    whole.wait()
    cut(places, chip, core, cores, stack_ref, chunks)
    for copy in copies:
        copy.wait()


def cut(places, chip, core, cores, stack_ref, chunks):
    halves, acq_share, _, tiles = stack_ref.shape[:4]
    for owners, chunk in zip(places, chunks):
        blocks = chunk.shape[0] // len(owners)
        for at, (turn, j) in enumerate(owners):
            owner = chip if turn is None else pick(turns_of(lax.axis_size("az"))[turn], chip)
            first = (owner * cores + (core ^ j)) * blocks
            for a in range(blocks):
                for half in range(halves):
                    for t in range(tiles):
                        for acq in range(acq_share):
                            chunk[at * blocks + a, half, t, acq] = stack_ref[
                                half, acq, first + a, t
                            ]


def prepare_kernel(
    acq_share, relative, groups, counts, list_ref, steer_ref, filter_ref,
    first_ref, half_op_ref, op_t_ref, wiener_ref, select_ref, chosen_ref, clear_ref, fmat_ref,
):
    group_count, _, acquisitions, elevation = steer_ref.shape
    blocks, columns, per_block = list_ref.shape
    depth = 2 * acquisitions
    pixels = chosen_ref.shape[0] * LANES
    first_group = lax.axis_index("rg") * group_count
    row = lax.broadcasted_iota(jnp.int32, (per_block, per_block), 0)
    lane = lax.broadcasted_iota(jnp.int32, (per_block, per_block), 1)
    entry = lax.broadcasted_iota(jnp.int32, (per_block, pixels), 0)
    pixel = lax.broadcasted_iota(jnp.int32, (per_block, pixels), 1)
    for a in range(blocks):
        for r in range(columns):
            listed = list_ref[a, r : r + 1].astype(F32)
            upright = jnp.sum(jnp.where(row == lane, listed, 0.0), axis=1, keepdims=True)
            usable = entry < counts[a : a + 1, r : r + 1]
            hit = (upright.astype(jnp.int32) == pixel) & usable
            chosen = jnp.where(hit, 1.0, 0.0).astype(F32)
            start = (a * columns + r) * per_block
            for t in range(pixels // LANES):
                part = chosen[:, t * LANES : (t + 1) * LANES]
                chosen_ref[t, start : start + per_block] = part.astype(BF16)
            covered = jnp.sum(chosen, axis=0, keepdims=True)
            clear_ref[a * columns + r] = jnp.broadcast_to(1.0 - covered, clear_ref.shape[1:])
    at = lax.broadcasted_iota(jnp.int32, (1, depth), 1)
    half, acq = at // acquisitions, at % acquisitions
    source = acq // acq_share
    if relative:
        cores, chips = lax.axis_size("acq"), lax.axis_size("az")
        chip, core = lax.axis_index("az"), lax.axis_index("acq")
        arrival = jnp.zeros_like(source)
        for turn, targets in enumerate(turns_of(chips)):
            sender = pick([targets.index(c) for c in range(chips)], chip)
            arrival = jnp.where(source // cores == sender, turn + 1, arrival)
        source = arrival * cores + ((source % cores) ^ core)
    place = ((source * 2 + half) * acq_share + acq % acq_share) * columns
    long = lax.broadcasted_iota(jnp.int32, (columns * depth, depth), 0)
    for r in range(columns):
        g = jnp.clip(jnp.max(groups[:, r : r + 1]) - first_group, 0, group_count - 1)
        select = jnp.where(long == place + r, 1.0, 0.0).astype(BF16)
        select_ref[r] = select
        real = steer_ref[g, 0]
        imag = steer_ref[g, 1]
        slabs = []
        for at in range(0, elevation, LANES):
            re, im = real[:, at : at + LANES], imag[:, at : at + LANES]
            slabs += [jnp.concatenate([re, im], axis=0), jnp.concatenate([-im, re], axis=0)]
        operator = jnp.concatenate(slabs, axis=1)
        half_op = operator * jnp.asarray(STEP_SIZE, BF16)
        first = dot(select, half_op).astype(BF16)
        op_t = jnp.transpose(operator.astype(F32)).astype(BF16)
        for slab in range(op_t_ref.shape[1]):
            op_t_ref[r, slab] = op_t[slab * 2 * LANES : (slab + 1) * 2 * LANES]
        for slab in range(len(slabs)):
            half_op_ref[r, slab] = half_op[:, slab * LANES : (slab + 1) * LANES]
            first_ref[r, slab] = first[:, slab * LANES : (slab + 1) * LANES]
        fmat_ref[:acquisitions, :acquisitions] = filter_ref[g, 0].astype(F32)
        fmat_ref[:acquisitions, acquisitions:] = -filter_ref[g, 1].astype(F32)
        fmat_ref[acquisitions:, :acquisitions] = filter_ref[g, 1].astype(F32)
        fmat_ref[acquisitions:, acquisitions:] = filter_ref[g, 0].astype(F32)
        spread = dot(fmat_ref[...].astype(BF16), select, (1, 1)).astype(BF16)
        wiener = dot(op_t, spread).astype(BF16)
        for slab in range(wiener_ref.shape[1]):
            wiener_ref[r, slab] = wiener[:, slab * LANES : (slab + 1) * LANES]


def wide(ref, *at):
    return jnp.concatenate([ref[where] for where in at], axis=-1)


def profile_body(
    grid, first_ref, half_op_ref, op_t_ref, wiener_ref, select_ref, chosen_ref, clear_ref,
    out_ref, real_ref, imag_ref, rounded_ref, target_ref, image_ref, sem,
):
    blocks, columns, elevation, _ = out_ref.shape
    tiles, entries = chosen_ref.shape[:2]
    per_block = entries // (blocks * columns)
    slabs = elevation // LANES

    def chosen(first, size):
        return wide(chosen_ref, *[(t, slice(first, first + size)) for t in range(tiles)])

    share = columns * per_block
    picked = [
        dot(chosen(a * share, share), grid(a), (1, 1)).astype(BF16) for a in range(blocks)
    ]
    picked = [
        jnp.concatenate([p[r * per_block : (r + 1) * per_block] for p in picked], axis=0)
        for r in range(columns)
    ]
    for r in range(columns):
        target_ref[r] = dot(picked[r], select_ref[r])

    def predicted(r):
        size = rounded_ref.shape[2]
        deep = op_t_ref.shape[2] // LANES
        total = None
        for at in range(0, op_t_ref.shape[1], 2):
            stacked = jnp.concatenate(
                [
                    wide(rounded_ref, *[(r, (at + j) * deep + k) for k in range(deep)])
                    for j in range(2)
                ],
                axis=0,
            )
            both = dot(stacked, wide(op_t_ref, (r, at), (r, at + 1)))
            total = both if total is None else total + both
        depth = op_t_ref.shape[3]
        return total[:size, :depth] + total[size:, depth:]

    def update(r, misfit, op_ref, first):
        for slab in range(slabs):
            z = dot(misfit, wide(op_ref, (r, 2 * slab), (r, 2 * slab + 1)))
            zr, zi = z[:, :LANES], z[:, LANES:]
            if not first:
                zr = zr + real_ref[r, slab]
                zi = zi + imag_ref[r, slab]
            magnitude = zr * zr + zi * zi
            factor = jnp.maximum(
                1.0 - SHRINK * lax.rsqrt(jnp.maximum(magnitude, SHRINK * SHRINK)), 0.0
            )
            xr = zr * factor
            xi = zi * factor
            real_ref[r, slab] = xr
            imag_ref[r, slab] = xi
            rounded_ref[r, 2 * slab] = xr.astype(BF16)
            rounded_ref[r, 2 * slab + 1] = xi.astype(BF16)

    shares = [
        (a, r, slab) for a in range(blocks) for slab in range(slabs) for r in range(columns)
    ]

    def wiener(a, r, slab):
        first = 2 * slab * LANES
        depths = range(wiener_ref.shape[1])
        br = dot(wide(wiener_ref, *[(r, k, slice(first, first + LANES)) for k in depths]), grid(a))
        first += LANES
        bi = dot(wide(wiener_ref, *[(r, k, slice(first, first + LANES)) for k in depths]), grid(a))
        power = (br * br + bi * bi) * clear_ref[a * columns + r, :1]
        power = power.astype(BF16)
        image_ref[a, r, slab * LANES : (slab + 1) * LANES] = power

    todo = list(shares)

    def more(count):
        for part in todo[:count]:
            wiener(*part)
        del todo[:count]

    for t in range(ITERS):
        if t == 0:
            misfits = picked
        else:
            misfits = [(target_ref[r] - predicted(r)).astype(BF16) for r in range(columns)]
        for r in range(columns):
            more(1)
            update(r, misfits[r], half_op_ref if t else first_ref, t == 0)

    def copies(a, r, slab):
        where = pl.ds(slab * LANES, LANES)
        return [
            pltpu.make_async_copy(image_ref.at[a, r, where], out_ref.at[a, r, where], sem)
        ]

    for r in range(columns):
        for a in range(blocks):
            rows = slice(a * per_block, (a + 1) * per_block)
            for slab in range(slabs):
                xr, xi = real_ref[r, slab, rows], imag_ref[r, slab, rows]
                strength = (xr * xr + xi * xi).astype(BF16)
                placed = dot(
                    strength, chosen((a * columns + r) * per_block, per_block), (0, 0)
                ).astype(BF16)
                where = slice(slab * LANES, (slab + 1) * LANES)
                image_ref[a, r, where] = image_ref[a, r, where] + placed
                for copy in copies(a, r, slab):
                    copy.start()
    for a in range(blocks):
        for r in range(columns):
            for slab in range(slabs):
                for copy in copies(a, r, slab):
                    copy.wait()


def join_kernel(skips, *refs):
    out_ref = refs[-1]
    at = 0
    for skip, ref in zip(skips, refs[:-1]):
        size = ref.shape[0] - skip
        out_ref[at : at + size] = ref[skip:]
        at += size


def pieces_kernel(count, order, *refs):
    pieces, rest = refs[:count], refs[count:]

    def grid(a):
        rows = []
        for at, lead in order:
            ref = pieces[at]
            where = lead + (a,) if len(ref.shape) == 6 else (a,)
            halves, tiles = ref.shape[-4:-2]
            for half in range(halves):
                rows.append(
                    jnp.concatenate(
                        [ref[where + (half, t)] for t in range(tiles)], axis=1
                    )
                )
        return jnp.concatenate(rows, axis=0)

    profile_body(grid, *rest)


def plain_kernel(pieces, *rest):
    profile_body(lambda a: pieces[a], *rest)


def shards(image_stack, steering, wiener_filter, range_group, lay_list, lay_count):
    halves, acq_share, azb_all, columns, pixels = image_stack.shape
    blocks = lay_list.shape[0]
    _, _, acquisitions, elevation = steering.shape
    depth = 2 * acquisitions
    chips = lax.axis_size("az")
    cores = lax.axis_size("acq")
    per_block = lay_list.shape[2]
    rows = blocks * per_block
    tiles = pixels // LANES
    slabs = 2 * elevation // LANES
    pairwise = acq_share * columns == 16 and cores == 2 and chips & (chips - 1) == 0
    small = [range_group.reshape(1, columns), lay_count, lay_list, steering, wiener_filter]

    def prepare(small):
        return pl.pallas_call(
            lambda *refs: prepare_kernel(acq_share, pairwise, *refs),
            out_shape=[
                jax.ShapeDtypeStruct((columns, slabs, columns * depth, LANES), BF16),
                jax.ShapeDtypeStruct((columns, slabs, depth, LANES), BF16),
                jax.ShapeDtypeStruct((columns, slabs // 2, 2 * LANES, depth), BF16),
                jax.ShapeDtypeStruct(
                    (columns, columns * depth // LANES, 2 * elevation, LANES), BF16
                ),
                jax.ShapeDtypeStruct((columns, columns * depth, depth), BF16),
                jax.ShapeDtypeStruct((tiles, blocks * columns * per_block, LANES), BF16),
                jax.ShapeDtypeStruct((blocks * columns, 8, pixels), F32),
            ],
            in_specs=[VMEM] * len(small),
            out_specs=[VMEM] * 7,
            scratch_shapes=[pltpu.VMEM((depth, depth), F32)],
            cost_estimate=pl.CostEstimate(
                flops=1_000_000_000, bytes_accessed=4_000_000, transcendentals=0
            ),
            compiler_params=pltpu.CompilerParams(vmem_limit_bytes=16 << 20),
            name="prepare",
        )(*small)

    if pairwise:
        view = image_stack.reshape(halves, acq_share, azb_all, columns, tiles, LANES)
        view = view.transpose(0, 1, 2, 4, 3, 5)
        turns = turns_of(chips)
        places = [[(None, 0)], [(None, 1)]]
        places += [[(turn, 0), (turn, 1)] for turn in range(len(turns))]
        unit = (halves, tiles, acq_share, columns, LANES)
        outputs = [
            jax.ShapeDtypeStruct((len(owners) * blocks,) + unit, BF16) for owners in places
        ]
        tiny = [x for x in small if x is not steering]
        relayed = pl.pallas_call(
            lambda *refs: relay_kernel(places, len(tiny), *refs),
            out_shape=outputs + [jax.ShapeDtypeStruct(x.shape, x.dtype) for x in tiny],
            in_specs=[HBM] * (1 + len(tiny)),
            out_specs=[VMEM] * (len(places) + len(tiny)),
            scratch_shapes=[
                pltpu.VMEM(view.shape, BF16),
                pltpu.SemaphoreType.DMA,
                pltpu.SemaphoreType.DMA((len(tiny),)),
            ],
            compiler_params=pltpu.CompilerParams(vmem_limit_bytes=4 << 20),
            name="relay",
        )(*[pltpu.with_memory_space_constraint(x, pltpu.HBM) for x in [view] + tiny])
        groups, counts, listed, filters = relayed[len(places) :]
        prepared = prepare([groups, counts, listed, steering, filters])
        flat = (halves, tiles, acq_share * columns, LANES)
        chunks = [chunk.reshape((-1,) + flat) for chunk in relayed[: len(places)]]
        got, waiting = {(0, 0): chunks[0]}, {(0, 1): chunks[1]}
        for at, (targets, chunk) in enumerate(zip(turns, chunks[2:])):
            arrived = lax.ppermute(chunk, "az", list(enumerate(targets)))
            got[at + 1, 0] = waiting[at + 1, 1] = arrived
        names = list(waiting)
        passed = []
        for group in (names[:2], names[2:]):
            skips = [waiting[n].shape[0] - blocks for n in group]
            passing = pl.pallas_call(
                lambda *refs: join_kernel(skips, *refs),
                out_shape=jax.ShapeDtypeStruct((len(group) * blocks,) + flat, BF16),
                in_specs=[VMEM] * len(group),
                out_specs=VMEM,
                compiler_params=pltpu.CompilerParams(vmem_limit_bytes=2 << 20),
                name="join",
            )(*[waiting[n] for n in group])
            if not passed:
                passing, prepared = lax.optimization_barrier((passing, prepared))
            array = lax.ppermute(passing, "acq", [(0, 1), (1, 0)])
            passed.append((group, array))
        arrays, order = [], {}
        for place, array in got.items():
            order[place] = (len(arrays), ())
            arrays.append(array)
        for group, array in passed:
            for at, place in enumerate(group):
                order[place] = (len(arrays), (at,))
            arrays.append(array.reshape((len(group), blocks) + flat))
        order = [order[d, j] for d in range(chips) for j in range(cores)]
        lead = arrays
        body = lambda *refs: pieces_kernel(len(arrays), order, *refs)
    else:
        moved = lax.all_to_all(
            image_stack, ("az", "acq"), split_axis=2, concat_axis=0, tiled=True
        )
        moved = moved.reshape(-1, acq_share, blocks, columns, pixels)
        lead = [moved.transpose(2, 0, 1, 3, 4).reshape(blocks, columns * depth, pixels)]
        body = plain_kernel
        prepared = prepare(small)

    return pl.pallas_call(
        body,
        out_shape=jax.ShapeDtypeStruct((blocks, columns, elevation, pixels), BF16),
        in_specs=[VMEM] * (len(lead) + len(prepared)),
        out_specs=ANY,
        scratch_shapes=[
            pltpu.VMEM((columns, slabs // 2, rows, LANES), F32),
            pltpu.VMEM((columns, slabs // 2, rows, LANES), F32),
            pltpu.VMEM((columns, slabs, rows, LANES), BF16),
            pltpu.VMEM((columns, rows, depth), F32),
            pltpu.VMEM((blocks, columns, elevation, pixels), BF16),
            pltpu.SemaphoreType.DMA,
        ],
        compiler_params=pltpu.CompilerParams(vmem_limit_bytes=24 << 20),
        cost_estimate=pl.CostEstimate(
            flops=2_000_000_000, bytes_accessed=4_000_000, transcendentals=0
        ),
        name="profiles",
    )(*lead, *prepared)


def solution(mesh):
    return jax.shard_map(
        shards,
        mesh=mesh,
        in_specs=(
            P(None, ("az", "acq"), "groups", "rg", None),
            P("rg", None, None, None),
            P("rg", None, None, None),
            P("rg"),
            P(("groups", "az", "acq"), "rg", None),
            P(("groups", "az", "acq"), "rg"),
        ),
        out_specs=P(("groups", "az", "acq"), "rg", None, None),
        check_vma=False,
    )
```

```python
import jax
import jax.numpy as jnp
from jax import lax
from jax.experimental import pallas as pl
from jax.experimental.pallas import tpu as pltpu
from jax.sharding import PartitionSpec as P

ITERS = 8
STEP_SIZE = 0.5
SHRINK = 0.25
LANES = 128
F32 = jnp.float32
BF16 = jnp.bfloat16

VMEM = pl.BlockSpec(memory_space=pltpu.VMEM)
ANY = pl.BlockSpec(memory_space=pl.ANY)
HBM = pl.BlockSpec(memory_space=pltpu.HBM)


def dot(a, b, contract=(1, 0)):
    return lax.dot_general(
        a, b, (((contract[0],), (contract[1],)), ((), ())), preferred_element_type=F32
    )


def turns_of(chips):
    if chips == 4:
        return [[1, 3, 0, 2], [3, 2, 1, 0], [2, 0, 3, 1]]
    far = sorted(range(1, chips), key=lambda d: (d < chips // 2, d))
    return [[c ^ d for c in range(chips)] for d in far]


def pick(table, index):
    return sum(jnp.where(index == at, value, 0) for at, value in enumerate(table))


def relay_kernel(places, x_ref, *refs):
    chunks, stack_ref, sem = refs[:-2], refs[-2], refs[-1]
    whole = pltpu.make_async_copy(x_ref, stack_ref, sem)
    whole.start()
    chip, core = lax.axis_index("az"), lax.axis_index("acq")
    cores = lax.axis_size("acq")
    whole.wait()
    cut(places, chip, core, cores, stack_ref, chunks)


def cut(places, chip, core, cores, stack_ref, chunks):
    halves, acq_share, _, tiles = stack_ref.shape[:4]
    for owners, chunk in zip(places, chunks):
        blocks = chunk.shape[0] // len(owners)
        for at, (turn, j) in enumerate(owners):
            owner = chip if turn is None else pick(turns_of(lax.axis_size("az"))[turn], chip)
            first = (owner * cores + (core ^ j)) * blocks
            for a in range(blocks):
                for half in range(halves):
                    for t in range(tiles):
                        for acq in range(acq_share):
                            chunk[at * blocks + a, half, t, acq] = stack_ref[
                                half, acq, first + a, t
                            ]


def prepare_kernel(
    acq_share, relative, groups_in, counts_in, list_in, steer_in, filter_in,
    first_ref, half_op_ref, op_t_ref, wiener_ref, select_ref, chosen_ref, clear_ref,
    fmat_ref, groups, counts, list_ref, steer_ref, filter_ref, sems,
):
    fetched = [
        pltpu.make_async_copy(source, target, sems.at[at])
        for at, (source, target) in enumerate(
            [
                (groups_in, groups), (counts_in, counts), (list_in, list_ref),
                (steer_in, steer_ref), (filter_in, filter_ref),
            ]
        )
    ]
    for copy in fetched:
        copy.start()
    for copy in fetched:
        copy.wait()

    group_count, _, acquisitions, elevation = steer_ref.shape
    blocks, columns, per_block = list_ref.shape
    depth = 2 * acquisitions
    pixels = chosen_ref.shape[0] * LANES
    first_group = lax.axis_index("rg") * group_count
    row = lax.broadcasted_iota(jnp.int32, (per_block, per_block), 0)
    lane = lax.broadcasted_iota(jnp.int32, (per_block, per_block), 1)
    entry = lax.broadcasted_iota(jnp.int32, (per_block, pixels), 0)
    pixel = lax.broadcasted_iota(jnp.int32, (per_block, pixels), 1)
    for a in range(blocks):
        for r in range(columns):
            listed = list_ref[a, r : r + 1].astype(F32)
            upright = jnp.sum(jnp.where(row == lane, listed, 0.0), axis=1, keepdims=True)
            usable = entry < counts[a : a + 1, r : r + 1]
            hit = (upright.astype(jnp.int32) == pixel) & usable
            chosen = jnp.where(hit, 1.0, 0.0).astype(F32)
            start = (a * columns + r) * per_block
            for t in range(pixels // LANES):
                part = chosen[:, t * LANES : (t + 1) * LANES]
                chosen_ref[t, start : start + per_block] = part.astype(BF16)
            covered = jnp.sum(chosen, axis=0, keepdims=True)
            clear_ref[a * columns + r] = jnp.broadcast_to(1.0 - covered, clear_ref.shape[1:])
    at = lax.broadcasted_iota(jnp.int32, (1, depth), 1)
    half, acq = at // acquisitions, at % acquisitions
    source = acq // acq_share
    if relative:
        cores, chips = lax.axis_size("acq"), lax.axis_size("az")
        chip, core = lax.axis_index("az"), lax.axis_index("acq")
        arrival = jnp.zeros_like(source)
        for turn, targets in enumerate(turns_of(chips)):
            sender = pick([targets.index(c) for c in range(chips)], chip)
            arrival = jnp.where(source // cores == sender, turn + 1, arrival)
        source = arrival * cores + ((source % cores) ^ core)
    place = ((source * 2 + half) * acq_share + acq % acq_share) * columns
    long = lax.broadcasted_iota(jnp.int32, (columns * depth, depth), 0)
    for r in range(columns):
        g = jnp.clip(jnp.max(groups[:, r : r + 1]) - first_group, 0, group_count - 1)
        select = jnp.where(long == place + r, 1.0, 0.0).astype(BF16)
        select_ref[r] = select
        real = steer_ref[g, 0]
        imag = steer_ref[g, 1]
        slabs = []
        for at in range(0, elevation, LANES):
            re, im = real[:, at : at + LANES], imag[:, at : at + LANES]
            slabs += [jnp.concatenate([re, im], axis=0), jnp.concatenate([-im, re], axis=0)]
        operator = jnp.concatenate(slabs, axis=1)
        half_op = operator * jnp.asarray(STEP_SIZE, BF16)
        first = dot(select, half_op).astype(BF16)
        op_t = jnp.transpose(operator.astype(F32)).astype(BF16)
        for slab in range(op_t_ref.shape[1]):
            op_t_ref[r, slab] = op_t[slab * 2 * LANES : (slab + 1) * 2 * LANES]
        for slab in range(len(slabs)):
            half_op_ref[r, slab] = half_op[:, slab * LANES : (slab + 1) * LANES]
            first_ref[r, slab] = first[:, slab * LANES : (slab + 1) * LANES]
        fmat_ref[:acquisitions, :acquisitions] = filter_ref[g, 0].astype(F32)
        fmat_ref[:acquisitions, acquisitions:] = -filter_ref[g, 1].astype(F32)
        fmat_ref[acquisitions:, :acquisitions] = filter_ref[g, 1].astype(F32)
        fmat_ref[acquisitions:, acquisitions:] = filter_ref[g, 0].astype(F32)
        spread = dot(fmat_ref[...].astype(BF16), select, (1, 1)).astype(BF16)
        wiener = dot(op_t, spread).astype(BF16)
        for slab in range(wiener_ref.shape[1]):
            wiener_ref[r, slab] = wiener[:, slab * LANES : (slab + 1) * LANES]


def wide(ref, *at):
    return jnp.concatenate([ref[where] for where in at], axis=-1)


def profile_body(
    grid, first_ref, half_op_ref, op_t_ref, wiener_ref, select_ref, chosen_ref, clear_ref,
    out_ref, real_ref, imag_ref, rounded_ref, target_ref, image_ref, sem,
):
    blocks, columns, elevation, _ = out_ref.shape
    tiles, entries = chosen_ref.shape[:2]
    per_block = entries // (blocks * columns)
    slabs = elevation // LANES

    def chosen(first, size):
        return wide(chosen_ref, *[(t, slice(first, first + size)) for t in range(tiles)])

    share = columns * per_block
    picked = [
        dot(chosen(a * share, share), grid(a), (1, 1)).astype(BF16) for a in range(blocks)
    ]
    picked = [
        jnp.concatenate([p[r * per_block : (r + 1) * per_block] for p in picked], axis=0)
        for r in range(columns)
    ]
    for r in range(columns):
        target_ref[r] = dot(picked[r], select_ref[r])

    def predicted(r):
        size = rounded_ref.shape[2]
        deep = op_t_ref.shape[2] // LANES
        total = None
        for at in range(0, op_t_ref.shape[1], 2):
            stacked = jnp.concatenate(
                [
                    wide(rounded_ref, *[(r, (at + j) * deep + k) for k in range(deep)])
                    for j in range(2)
                ],
                axis=0,
            )
            both = dot(stacked, wide(op_t_ref, (r, at), (r, at + 1)))
            total = both if total is None else total + both
        depth = op_t_ref.shape[3]
        return total[:size, :depth] + total[size:, depth:]

    def update(r, misfit, op_ref, first):
        for slab in range(slabs):
            z = dot(misfit, wide(op_ref, (r, 2 * slab), (r, 2 * slab + 1)))
            zr, zi = z[:, :LANES], z[:, LANES:]
            if not first:
                zr = zr + real_ref[r, slab]
                zi = zi + imag_ref[r, slab]
            magnitude = zr * zr + zi * zi
            factor = jnp.maximum(
                1.0 - SHRINK * lax.rsqrt(jnp.maximum(magnitude, SHRINK * SHRINK)), 0.0
            )
            xr = zr * factor
            xi = zi * factor
            real_ref[r, slab] = xr
            imag_ref[r, slab] = xi
            rounded_ref[r, 2 * slab] = xr.astype(BF16)
            rounded_ref[r, 2 * slab + 1] = xi.astype(BF16)

    shares = [
        (a, r, slab) for a in range(blocks) for slab in range(slabs) for r in range(columns)
    ]

    def wiener(a, r, slab):
        first = 2 * slab * LANES
        depths = range(wiener_ref.shape[1])
        br = dot(wide(wiener_ref, *[(r, k, slice(first, first + LANES)) for k in depths]), grid(a))
        first += LANES
        bi = dot(wide(wiener_ref, *[(r, k, slice(first, first + LANES)) for k in depths]), grid(a))
        power = (br * br + bi * bi) * clear_ref[a * columns + r, :1]
        power = power.astype(BF16)
        image_ref[a, r, slab * LANES : (slab + 1) * LANES] = power

    todo = list(shares)

    def more(count):
        for part in todo[:count]:
            wiener(*part)
        del todo[:count]

    for t in range(ITERS):
        if t == 0:
            misfits = picked
        else:
            misfits = [(target_ref[r] - predicted(r)).astype(BF16) for r in range(columns)]
        for r in range(columns):
            more(1)
            update(r, misfits[r], half_op_ref if t else first_ref, t == 0)

    def copies(a, r, slab):
        where = pl.ds(slab * LANES, LANES)
        return [
            pltpu.make_async_copy(image_ref.at[a, r, where], out_ref.at[a, r, where], sem)
        ]

    for r in range(columns):
        for a in range(blocks):
            rows = slice(a * per_block, (a + 1) * per_block)
            for slab in range(slabs):
                xr, xi = real_ref[r, slab, rows], imag_ref[r, slab, rows]
                strength = (xr * xr + xi * xi).astype(BF16)
                placed = dot(
                    strength, chosen((a * columns + r) * per_block, per_block), (0, 0)
                ).astype(BF16)
                where = slice(slab * LANES, (slab + 1) * LANES)
                image_ref[a, r, where] = image_ref[a, r, where] + placed
                for copy in copies(a, r, slab):
                    copy.start()
    for a in range(blocks):
        for r in range(columns):
            for slab in range(slabs):
                for copy in copies(a, r, slab):
                    copy.wait()


def join_kernel(skips, *refs):
    out_ref = refs[-1]
    at = 0
    for skip, ref in zip(skips, refs[:-1]):
        size = ref.shape[0] - skip
        out_ref[at : at + size] = ref[skip:]
        at += size


def pieces_kernel(count, order, *refs):
    pieces, rest = refs[:count], refs[count:]

    def grid(a):
        rows = []
        for at, lead in order:
            ref = pieces[at]
            where = lead + (a,) if len(ref.shape) == 6 else (a,)
            halves, tiles = ref.shape[-4:-2]
            for half in range(halves):
                rows.append(
                    jnp.concatenate(
                        [ref[where + (half, t)] for t in range(tiles)], axis=1
                    )
                )
        return jnp.concatenate(rows, axis=0)

    profile_body(grid, *rest)


def plain_kernel(pieces, *rest):
    profile_body(lambda a: pieces[a], *rest)


def shards(image_stack, steering, wiener_filter, range_group, lay_list, lay_count):
    halves, acq_share, azb_all, columns, pixels = image_stack.shape
    blocks = lay_list.shape[0]
    _, _, acquisitions, elevation = steering.shape
    depth = 2 * acquisitions
    chips = lax.axis_size("az")
    cores = lax.axis_size("acq")
    per_block = lay_list.shape[2]
    rows = blocks * per_block
    tiles = pixels // LANES
    slabs = 2 * elevation // LANES
    pairwise = acq_share * columns == 16 and cores == 2 and chips & (chips - 1) == 0
    small = [range_group.reshape(1, columns), lay_count, lay_list, steering, wiener_filter]

    def prepare(small):
        return pl.pallas_call(
            lambda *refs: prepare_kernel(acq_share, pairwise, *refs),
            out_shape=[
                jax.ShapeDtypeStruct((columns, slabs, columns * depth, LANES), BF16),
                jax.ShapeDtypeStruct((columns, slabs, depth, LANES), BF16),
                jax.ShapeDtypeStruct((columns, slabs // 2, 2 * LANES, depth), BF16),
                jax.ShapeDtypeStruct(
                    (columns, columns * depth // LANES, 2 * elevation, LANES), BF16
                ),
                jax.ShapeDtypeStruct((columns, columns * depth, depth), BF16),
                jax.ShapeDtypeStruct((tiles, blocks * columns * per_block, LANES), BF16),
                jax.ShapeDtypeStruct((blocks * columns, 8, pixels), F32),
            ],
            in_specs=[HBM] * len(small),
            out_specs=[VMEM] * 7,
            scratch_shapes=[pltpu.VMEM((depth, depth), F32)]
            + [pltpu.VMEM(x.shape, x.dtype) for x in small]
            + [pltpu.SemaphoreType.DMA((len(small),))],
            cost_estimate=pl.CostEstimate(
                flops=1_000_000_000, bytes_accessed=4_000_000, transcendentals=0
            ),
            compiler_params=pltpu.CompilerParams(vmem_limit_bytes=16 << 20),
            name="prepare",
        )(*[pltpu.with_memory_space_constraint(x, pltpu.HBM) for x in small])

    if pairwise:
        view = image_stack.reshape(halves, acq_share, azb_all, columns, tiles, LANES)
        view = view.transpose(0, 1, 2, 4, 3, 5)
        turns = turns_of(chips)
        places = [[(None, 0)], [(None, 1)]]
        places += [[(turn, 0), (turn, 1)] for turn in range(len(turns))]
        unit = (halves, tiles, acq_share, columns, LANES)
        outputs = [
            jax.ShapeDtypeStruct((len(owners) * blocks,) + unit, BF16) for owners in places
        ]
        relayed = pl.pallas_call(
            lambda *refs: relay_kernel(places, *refs),
            out_shape=outputs,
            in_specs=[HBM],
            out_specs=[VMEM] * len(places),
            scratch_shapes=[pltpu.VMEM(view.shape, BF16), pltpu.SemaphoreType.DMA],
            compiler_params=pltpu.CompilerParams(vmem_limit_bytes=4 << 20),
            name="relay",
        )(pltpu.with_memory_space_constraint(view, pltpu.HBM))
        prepared = prepare(small)
        flat = (halves, tiles, acq_share * columns, LANES)
        chunks = [chunk.reshape((-1,) + flat) for chunk in relayed]
        got, waiting = {(0, 0): chunks[0]}, {(0, 1): chunks[1]}
        for at, (targets, chunk) in enumerate(zip(turns, chunks[2:])):
            arrived = lax.ppermute(chunk, "az", list(enumerate(targets)))
            got[at + 1, 0] = waiting[at + 1, 1] = arrived
        names = list(waiting)
        passed = []
        for group in (names[:2], names[2:]):
            skips = [waiting[n].shape[0] - blocks for n in group]
            passing = pl.pallas_call(
                lambda *refs: join_kernel(skips, *refs),
                out_shape=jax.ShapeDtypeStruct((len(group) * blocks,) + flat, BF16),
                in_specs=[VMEM] * len(group),
                out_specs=VMEM,
                compiler_params=pltpu.CompilerParams(vmem_limit_bytes=2 << 20),
                name="join",
            )(*[waiting[n] for n in group])
            if not passed:
                passing, prepared = lax.optimization_barrier((passing, prepared))
            array = lax.ppermute(passing, "acq", [(0, 1), (1, 0)])
            passed.append((group, array))
        arrays, order = [], {}
        for place, array in got.items():
            order[place] = (len(arrays), ())
            arrays.append(array)
        for group, array in passed:
            for at, place in enumerate(group):
                order[place] = (len(arrays), (at,))
            arrays.append(array.reshape((len(group), blocks) + flat))
        order = [order[d, j] for d in range(chips) for j in range(cores)]
        lead = arrays
        body = lambda *refs: pieces_kernel(len(arrays), order, *refs)
    else:
        moved = lax.all_to_all(
            image_stack, ("az", "acq"), split_axis=2, concat_axis=0, tiled=True
        )
        moved = moved.reshape(-1, acq_share, blocks, columns, pixels)
        lead = [moved.transpose(2, 0, 1, 3, 4).reshape(blocks, columns * depth, pixels)]
        body = plain_kernel
        prepared = prepare(small)

    return pl.pallas_call(
        body,
        out_shape=jax.ShapeDtypeStruct((blocks, columns, elevation, pixels), BF16),
        in_specs=[VMEM] * (len(lead) + len(prepared)),
        out_specs=ANY,
        scratch_shapes=[
            pltpu.VMEM((columns, slabs // 2, rows, LANES), F32),
            pltpu.VMEM((columns, slabs // 2, rows, LANES), F32),
            pltpu.VMEM((columns, slabs, rows, LANES), BF16),
            pltpu.VMEM((columns, rows, depth), F32),
            pltpu.VMEM((blocks, columns, elevation, pixels), BF16),
            pltpu.SemaphoreType.DMA,
        ],
        compiler_params=pltpu.CompilerParams(vmem_limit_bytes=24 << 20),
        cost_estimate=pl.CostEstimate(
            flops=2_000_000_000, bytes_accessed=4_000_000, transcendentals=0
        ),
        name="profiles",
    )(*lead, *prepared)


def solution(mesh):
    return jax.shard_map(
        shards,
        mesh=mesh,
        in_specs=(
            P(None, ("az", "acq"), "groups", "rg", None),
            P("rg", None, None, None),
            P("rg", None, None, None),
            P("rg"),
            P(("groups", "az", "acq"), "rg", None),
            P(("groups", "az", "acq"), "rg"),
        ),
        out_specs=P(("groups", "az", "acq"), "rg", None, None),
        check_vma=False,
    )
```

```python
import jax
import jax.numpy as jnp
from jax import lax
from jax.experimental import pallas as pl
from jax.experimental.pallas import tpu as pltpu
from jax.sharding import PartitionSpec as P

ITERS = 8
STEP_SIZE = 0.5
SHRINK = 0.25
LANES = 128
F32 = jnp.float32
BF16 = jnp.bfloat16

VMEM = pl.BlockSpec(memory_space=pltpu.VMEM)
ANY = pl.BlockSpec(memory_space=pl.ANY)
HBM = pl.BlockSpec(memory_space=pltpu.HBM)


def dot(a, b, contract=(1, 0)):
    return lax.dot_general(
        a, b, (((contract[0],), (contract[1],)), ((), ())), preferred_element_type=F32
    )


def turns_of(chips):
    if chips == 4:
        return [[1, 3, 0, 2], [3, 2, 1, 0], [2, 0, 3, 1]]
    far = sorted(range(1, chips), key=lambda d: (d < chips // 2, d))
    return [[c ^ d for c in range(chips)] for d in far]


def pick(table, index):
    return sum(jnp.where(index == at, value, 0) for at, value in enumerate(table))


def relay_kernel(places, x_ref, *refs):
    chunks, stack_ref, sem = refs[:-2], refs[-2], refs[-1]
    parts = [
        pltpu.make_async_copy(x_ref.at[half, at], stack_ref.at[half, at], sem)
        for half in range(x_ref.shape[0])
        for at in range(x_ref.shape[1])
    ]
    for part in parts:
        part.start()
    chip, core = lax.axis_index("az"), lax.axis_index("acq")
    cores = lax.axis_size("acq")
    for part in parts:
        part.wait()
    cut(places, chip, core, cores, stack_ref, chunks)


def cut(places, chip, core, cores, stack_ref, chunks):
    halves, acq_share, _, tiles = stack_ref.shape[:4]
    for owners, chunk in zip(places, chunks):
        blocks = chunk.shape[0] // len(owners)
        for at, (turn, j) in enumerate(owners):
            owner = chip if turn is None else pick(turns_of(lax.axis_size("az"))[turn], chip)
            first = (owner * cores + (core ^ j)) * blocks
            for a in range(blocks):
                for half in range(halves):
                    for t in range(tiles):
                        for acq in range(acq_share):
                            chunk[at * blocks + a, half, t, acq] = stack_ref[
                                half, acq, first + a, t
                            ]


def prepare_kernel(
    acq_share, relative, groups_in, counts_in, list_in, steer_in, filter_in,
    first_ref, half_op_ref, op_t_ref, wiener_ref, select_ref, chosen_ref, clear_ref,
    fmat_ref, groups, counts, list_ref, steer_ref, filter_ref, sems,
):
    fetched = [
        pltpu.make_async_copy(source, target, sems.at[at])
        for at, (source, target) in enumerate(
            [
                (groups_in, groups), (counts_in, counts), (list_in, list_ref),
                (steer_in, steer_ref), (filter_in, filter_ref),
            ]
        )
    ]
    for copy in fetched:
        copy.start()
    for copy in fetched:
        copy.wait()

    group_count, _, acquisitions, elevation = steer_ref.shape
    blocks, columns, per_block = list_ref.shape
    depth = 2 * acquisitions
    pixels = chosen_ref.shape[0] * LANES
    first_group = lax.axis_index("rg") * group_count
    row = lax.broadcasted_iota(jnp.int32, (per_block, per_block), 0)
    lane = lax.broadcasted_iota(jnp.int32, (per_block, per_block), 1)
    entry = lax.broadcasted_iota(jnp.int32, (per_block, pixels), 0)
    pixel = lax.broadcasted_iota(jnp.int32, (per_block, pixels), 1)
    for a in range(blocks):
        for r in range(columns):
            listed = list_ref[a, r : r + 1].astype(F32)
            upright = jnp.sum(jnp.where(row == lane, listed, 0.0), axis=1, keepdims=True)
            usable = entry < counts[a : a + 1, r : r + 1]
            hit = (upright.astype(jnp.int32) == pixel) & usable
            chosen = jnp.where(hit, 1.0, 0.0).astype(F32)
            start = (a * columns + r) * per_block
            for t in range(pixels // LANES):
                part = chosen[:, t * LANES : (t + 1) * LANES]
                chosen_ref[t, start : start + per_block] = part.astype(BF16)
            covered = jnp.sum(chosen, axis=0, keepdims=True)
            clear_ref[a * columns + r] = jnp.broadcast_to(1.0 - covered, clear_ref.shape[1:])
    at = lax.broadcasted_iota(jnp.int32, (1, depth), 1)
    half, acq = at // acquisitions, at % acquisitions
    source = acq // acq_share
    if relative:
        cores, chips = lax.axis_size("acq"), lax.axis_size("az")
        chip, core = lax.axis_index("az"), lax.axis_index("acq")
        arrival = jnp.zeros_like(source)
        for turn, targets in enumerate(turns_of(chips)):
            sender = pick([targets.index(c) for c in range(chips)], chip)
            arrival = jnp.where(source // cores == sender, turn + 1, arrival)
        source = arrival * cores + ((source % cores) ^ core)
    place = ((source * 2 + half) * acq_share + acq % acq_share) * columns
    long = lax.broadcasted_iota(jnp.int32, (columns * depth, depth), 0)
    for r in range(columns):
        g = jnp.clip(jnp.max(groups[:, r : r + 1]) - first_group, 0, group_count - 1)
        select = jnp.where(long == place + r, 1.0, 0.0).astype(BF16)
        select_ref[r] = select
        real = steer_ref[g, 0]
        imag = steer_ref[g, 1]
        slabs = []
        for at in range(0, elevation, LANES):
            re, im = real[:, at : at + LANES], imag[:, at : at + LANES]
            slabs += [jnp.concatenate([re, im], axis=0), jnp.concatenate([-im, re], axis=0)]
        operator = jnp.concatenate(slabs, axis=1)
        half_op = operator * jnp.asarray(STEP_SIZE, BF16)
        first = dot(select, half_op).astype(BF16)
        op_t = jnp.transpose(operator.astype(F32)).astype(BF16)
        for slab in range(op_t_ref.shape[1]):
            op_t_ref[r, slab] = op_t[slab * 2 * LANES : (slab + 1) * 2 * LANES]
        for slab in range(len(slabs)):
            half_op_ref[r, slab] = half_op[:, slab * LANES : (slab + 1) * LANES]
            first_ref[r, slab] = first[:, slab * LANES : (slab + 1) * LANES]
        fmat_ref[:acquisitions, :acquisitions] = filter_ref[g, 0].astype(F32)
        fmat_ref[:acquisitions, acquisitions:] = -filter_ref[g, 1].astype(F32)
        fmat_ref[acquisitions:, :acquisitions] = filter_ref[g, 1].astype(F32)
        fmat_ref[acquisitions:, acquisitions:] = filter_ref[g, 0].astype(F32)
        spread = dot(fmat_ref[...].astype(BF16), select, (1, 1)).astype(BF16)
        wiener = dot(op_t, spread).astype(BF16)
        for slab in range(wiener_ref.shape[1]):
            wiener_ref[r, slab] = wiener[:, slab * LANES : (slab + 1) * LANES]


def wide(ref, *at):
    return jnp.concatenate([ref[where] for where in at], axis=-1)


def profile_body(
    grid, first_ref, half_op_ref, op_t_ref, wiener_ref, select_ref, chosen_ref, clear_ref,
    out_ref, real_ref, imag_ref, rounded_ref, target_ref, image_ref, sem,
):
    blocks, columns, elevation, _ = out_ref.shape
    tiles, entries = chosen_ref.shape[:2]
    per_block = entries // (blocks * columns)
    slabs = elevation // LANES

    def chosen(first, size):
        return wide(chosen_ref, *[(t, slice(first, first + size)) for t in range(tiles)])

    share = columns * per_block
    picked = [
        dot(chosen(a * share, share), grid(a), (1, 1)).astype(BF16) for a in range(blocks)
    ]
    picked = [
        jnp.concatenate([p[r * per_block : (r + 1) * per_block] for p in picked], axis=0)
        for r in range(columns)
    ]
    for r in range(columns):
        target_ref[r] = dot(picked[r], select_ref[r])

    def predicted(r):
        size = rounded_ref.shape[2]
        deep = op_t_ref.shape[2] // LANES
        total = None
        for at in range(0, op_t_ref.shape[1], 2):
            stacked = jnp.concatenate(
                [
                    wide(rounded_ref, *[(r, (at + j) * deep + k) for k in range(deep)])
                    for j in range(2)
                ],
                axis=0,
            )
            both = dot(stacked, wide(op_t_ref, (r, at), (r, at + 1)))
            total = both if total is None else total + both
        depth = op_t_ref.shape[3]
        return total[:size, :depth] + total[size:, depth:]

    def update(r, misfit, op_ref, first):
        for slab in range(slabs):
            z = dot(misfit, wide(op_ref, (r, 2 * slab), (r, 2 * slab + 1)))
            zr, zi = z[:, :LANES], z[:, LANES:]
            if not first:
                zr = zr + real_ref[r, slab]
                zi = zi + imag_ref[r, slab]
            magnitude = zr * zr + zi * zi
            factor = jnp.maximum(
                1.0 - SHRINK * lax.rsqrt(jnp.maximum(magnitude, SHRINK * SHRINK)), 0.0
            )
            xr = zr * factor
            xi = zi * factor
            real_ref[r, slab] = xr
            imag_ref[r, slab] = xi
            rounded_ref[r, 2 * slab] = xr.astype(BF16)
            rounded_ref[r, 2 * slab + 1] = xi.astype(BF16)

    shares = [
        (a, r, slab) for a in range(blocks) for slab in range(slabs) for r in range(columns)
    ]

    def wiener(a, r, slab):
        first = 2 * slab * LANES
        depths = range(wiener_ref.shape[1])
        br = dot(wide(wiener_ref, *[(r, k, slice(first, first + LANES)) for k in depths]), grid(a))
        first += LANES
        bi = dot(wide(wiener_ref, *[(r, k, slice(first, first + LANES)) for k in depths]), grid(a))
        power = (br * br + bi * bi) * clear_ref[a * columns + r, :1]
        power = power.astype(BF16)
        image_ref[a, r, slab * LANES : (slab + 1) * LANES] = power

    todo = list(shares)

    def more(count):
        for part in todo[:count]:
            wiener(*part)
        del todo[:count]

    for t in range(ITERS):
        if t == 0:
            misfits = picked
        else:
            misfits = [(target_ref[r] - predicted(r)).astype(BF16) for r in range(columns)]
        for r in range(columns):
            more(1)
            update(r, misfits[r], half_op_ref if t else first_ref, t == 0)

    def copies(a, r, slab):
        where = pl.ds(slab * LANES, LANES)
        return [
            pltpu.make_async_copy(image_ref.at[a, r, where], out_ref.at[a, r, where], sem)
        ]

    for r in range(columns):
        for slab in range(slabs):
            for a in range(blocks):
                rows = slice(a * per_block, (a + 1) * per_block)
                xr, xi = real_ref[r, slab, rows], imag_ref[r, slab, rows]
                strength = (xr * xr + xi * xi).astype(BF16)
                placed = dot(
                    strength, chosen((a * columns + r) * per_block, per_block), (0, 0)
                ).astype(BF16)
                where = slice(slab * LANES, (slab + 1) * LANES)
                image_ref[a, r, where] = image_ref[a, r, where] + placed
                for copy in copies(a, r, slab):
                    copy.start()
    for a in range(blocks):
        for r in range(columns):
            for slab in range(slabs):
                for copy in copies(a, r, slab):
                    copy.wait()


def join_kernel(skips, *refs):
    out_ref = refs[-1]
    at = 0
    for skip, ref in zip(skips, refs[:-1]):
        size = ref.shape[0] - skip
        out_ref[at : at + size] = ref[skip:]
        at += size


def pieces_kernel(count, order, *refs):
    pieces, rest = refs[:count], refs[count:]

    def grid(a):
        rows = []
        for at, lead in order:
            ref = pieces[at]
            where = lead + (a,) if len(ref.shape) == 6 else (a,)
            halves, tiles = ref.shape[-4:-2]
            for half in range(halves):
                rows.append(
                    jnp.concatenate(
                        [ref[where + (half, t)] for t in range(tiles)], axis=1
                    )
                )
        return jnp.concatenate(rows, axis=0)

    profile_body(grid, *rest)


def plain_kernel(pieces, *rest):
    profile_body(lambda a: pieces[a], *rest)


def shards(image_stack, steering, wiener_filter, range_group, lay_list, lay_count):
    halves, acq_share, azb_all, columns, pixels = image_stack.shape
    blocks = lay_list.shape[0]
    _, _, acquisitions, elevation = steering.shape
    depth = 2 * acquisitions
    chips = lax.axis_size("az")
    cores = lax.axis_size("acq")
    per_block = lay_list.shape[2]
    rows = blocks * per_block
    tiles = pixels // LANES
    slabs = 2 * elevation // LANES
    pairwise = acq_share * columns == 16 and cores == 2 and chips & (chips - 1) == 0
    small = [range_group.reshape(1, columns), lay_count, lay_list, steering, wiener_filter]

    def prepare(small):
        return pl.pallas_call(
            lambda *refs: prepare_kernel(acq_share, pairwise, *refs),
            out_shape=[
                jax.ShapeDtypeStruct((columns, slabs, columns * depth, LANES), BF16),
                jax.ShapeDtypeStruct((columns, slabs, depth, LANES), BF16),
                jax.ShapeDtypeStruct((columns, slabs // 2, 2 * LANES, depth), BF16),
                jax.ShapeDtypeStruct(
                    (columns, columns * depth // LANES, 2 * elevation, LANES), BF16
                ),
                jax.ShapeDtypeStruct((columns, columns * depth, depth), BF16),
                jax.ShapeDtypeStruct((tiles, blocks * columns * per_block, LANES), BF16),
                jax.ShapeDtypeStruct((blocks * columns, 8, pixels), F32),
            ],
            in_specs=[HBM] * len(small),
            out_specs=[VMEM] * 7,
            scratch_shapes=[pltpu.VMEM((depth, depth), F32)]
            + [pltpu.VMEM(x.shape, x.dtype) for x in small]
            + [pltpu.SemaphoreType.DMA((len(small),))],
            cost_estimate=pl.CostEstimate(
                flops=1_000_000_000, bytes_accessed=4_000_000, transcendentals=0
            ),
            compiler_params=pltpu.CompilerParams(vmem_limit_bytes=16 << 20),
            name="prepare",
        )(*[pltpu.with_memory_space_constraint(x, pltpu.HBM) for x in small])

    if pairwise:
        view = image_stack.reshape(halves, acq_share, azb_all, columns, tiles, LANES)
        view = view.transpose(0, 1, 2, 4, 3, 5)
        turns = turns_of(chips)
        places = [[(None, 0)], [(None, 1)]]
        places += [[(turn, 0), (turn, 1)] for turn in range(len(turns))]
        unit = (halves, tiles, acq_share, columns, LANES)
        outputs = [
            jax.ShapeDtypeStruct((len(owners) * blocks,) + unit, BF16) for owners in places
        ]
        relayed = pl.pallas_call(
            lambda *refs: relay_kernel(places, *refs),
            out_shape=outputs,
            in_specs=[HBM],
            out_specs=[VMEM] * len(places),
            scratch_shapes=[pltpu.VMEM(view.shape, BF16), pltpu.SemaphoreType.DMA],
            compiler_params=pltpu.CompilerParams(vmem_limit_bytes=4 << 20),
            name="relay",
        )(pltpu.with_memory_space_constraint(view, pltpu.HBM))
        prepared = prepare(small)
        flat = (halves, tiles, acq_share * columns, LANES)
        chunks = [chunk.reshape((-1,) + flat) for chunk in relayed]
        got, waiting = {(0, 0): chunks[0]}, {(0, 1): chunks[1]}
        for at, (targets, chunk) in enumerate(zip(turns, chunks[2:])):
            arrived = lax.ppermute(chunk, "az", list(enumerate(targets)))
            got[at + 1, 0] = waiting[at + 1, 1] = arrived
        names = list(waiting)
        passed = []
        for group in (names[:2], names[2:]):
            skips = [waiting[n].shape[0] - blocks for n in group]
            passing = pl.pallas_call(
                lambda *refs: join_kernel(skips, *refs),
                out_shape=jax.ShapeDtypeStruct((len(group) * blocks,) + flat, BF16),
                in_specs=[VMEM] * len(group),
                out_specs=VMEM,
                compiler_params=pltpu.CompilerParams(vmem_limit_bytes=2 << 20),
                name="join",
            )(*[waiting[n] for n in group])
            if not passed:
                passing, prepared = lax.optimization_barrier((passing, prepared))
            array = lax.ppermute(passing, "acq", [(0, 1), (1, 0)])
            passed.append((group, array))
        arrays, order = [], {}
        for place, array in got.items():
            order[place] = (len(arrays), ())
            arrays.append(array)
        for group, array in passed:
            for at, place in enumerate(group):
                order[place] = (len(arrays), (at,))
            arrays.append(array.reshape((len(group), blocks) + flat))
        order = [order[d, j] for d in range(chips) for j in range(cores)]
        lead = arrays
        body = lambda *refs: pieces_kernel(len(arrays), order, *refs)
    else:
        moved = lax.all_to_all(
            image_stack, ("az", "acq"), split_axis=2, concat_axis=0, tiled=True
        )
        moved = moved.reshape(-1, acq_share, blocks, columns, pixels)
        lead = [moved.transpose(2, 0, 1, 3, 4).reshape(blocks, columns * depth, pixels)]
        body = plain_kernel
        prepared = prepare(small)

    return pl.pallas_call(
        body,
        out_shape=jax.ShapeDtypeStruct((blocks, columns, elevation, pixels), BF16),
        in_specs=[VMEM] * (len(lead) + len(prepared)),
        out_specs=ANY,
        scratch_shapes=[
            pltpu.VMEM((columns, slabs // 2, rows, LANES), F32),
            pltpu.VMEM((columns, slabs // 2, rows, LANES), F32),
            pltpu.VMEM((columns, slabs, rows, LANES), BF16),
            pltpu.VMEM((columns, rows, depth), F32),
            pltpu.VMEM((blocks, columns, elevation, pixels), BF16),
            pltpu.SemaphoreType.DMA,
        ],
        compiler_params=pltpu.CompilerParams(vmem_limit_bytes=24 << 20),
        cost_estimate=pl.CostEstimate(
            flops=2_000_000_000, bytes_accessed=4_000_000, transcendentals=0
        ),
        name="profiles",
    )(*lead, *prepared)


def solution(mesh):
    return jax.shard_map(
        shards,
        mesh=mesh,
        in_specs=(
            P(None, ("az", "acq"), "groups", "rg", None),
            P("rg", None, None, None),
            P("rg", None, None, None),
            P("rg"),
            P(("groups", "az", "acq"), "rg", None),
            P(("groups", "az", "acq"), "rg"),
        ),
        out_specs=P(("groups", "az", "acq"), "rg", None, None),
        check_vma=False,
    )
```
